256 devices in a mesh: grp: 2 (over z), seq: 128 (over y, x, core).
Axes of the slice: x: 8, y: 8, z: 2, core: 2. Of those that a mesh axis runs over, the one named last changes fastest.
The devices are a block of a 8x8x16 slice.
Arguments:
- queries: bfloat16 [256, 4096], P(('grp', 'seq')), parts along dimension 0, may hold values from -9 to 9
- question_keys: bfloat16 [256, 2048], P(('grp', 'seq')), parts along dimension 0, may hold values from -4 to 4
- question_values: bfloat16 [256, 2048], P(('grp', 'seq')), parts along dimension 0, may hold values from -5 to 5
- doc_keys: bfloat16 [131072, 2048], P(('grp', 'seq')), parts along dimension 0, may hold values from -4 to 4
- doc_values: bfloat16 [131072, 2048], P(('grp', 'seq')), parts along dimension 0, may hold values from -5 to 5
- lengths: int32 [2], P('grp'), parts along dimension 0, may hold values from 4 to 128
- offsets: int32 [2], P('grp'), parts along dimension 0, may hold values from 2 to 65536, as said below
Outputs:
- attended: bfloat16 [256, 4096], P(('grp', 'seq')), parts along dimension 0
The draws below stay inside these ranges and needn't reach their ends.
There are 2 independent parts, one for each index of `grp`. The reference program is written for one: setup_inputs(seed, part) draws one part's arguments, and reference() takes and returns one part's arrays. A program takes and returns all parts, laid end to end along the dimension named above; each array names one. Nothing has to cross between parts.
Inputs may be any that keep to these rules, and one draw needn't show every extreme that they name: Some question has offsets equal to 65536.
All inputs are finite; a program needn't handle non-finite values.
Results may differ from the reference program's by a relative error of at most 0.0029.
Values may be sent and summed in bfloat16 or wider, within the bound.
A program may use at most 64 MiB of HBM per device.

```python
import jax
import jax.numpy as jnp
from jax import lax

H = 32
KVH = 16
HD = 128
QSCALE = 144
QL = 128
NQ = 1
DOC_DEV = 512
QT = 128
DOC = 65536
N_SEQ = 128


def draw_queries(key, part):
    values = 3.0 * jax.random.normal(jax.random.fold_in(key, 11), (NQ * QL, H * HD), jnp.float32)
    values = jnp.clip(values, -9.0, 9.0)
    return values.astype(jnp.bfloat16)


def draw_doc_keys(key, part):
    values = jax.random.normal(jax.random.fold_in(key, 13), (DOC, KVH * HD), jnp.float32)
    values = jnp.clip(values, -4.0, 4.0)
    return values.astype(jnp.bfloat16)


def draw_offsets(key, part):
    spread = jax.random.randint(jax.random.fold_in(key, 3), (NQ,), 0, DOC - 1)
    shifts = jax.random.randint(jax.random.fold_in(key, 5), (NQ,), 0, 11)
    result = 2 + jnp.right_shift(spread, shifts)
    chosen = jax.random.randint(jax.random.fold_in(key, 9), (), 0, NQ)
    result = jnp.where(jnp.arange(NQ, dtype=jnp.int32) == chosen, DOC, result)
    return result.astype(jnp.int32)


def levels(rng, dims, split, least, top_value):
    def one(dim, parts):
        heights = jax.random.uniform(jax.random.fold_in(jax.random.fold_in(rng, 6), dim), (parts,), jnp.float32, least / len(split), top_value / len(split))
        return jnp.repeat(jnp.exp(heights), dims[dim] // parts).reshape((-1,) + (1,) * (len(dims) - dim - 1))

    loudness = one(*split[0])
    for cut in split[1:]:
        loudness = loudness * one(*cut)
    return loudness


def normal_values(key, dims, width, most, shards=(), held_as=jnp.bfloat16):
    values = width * jax.random.normal(key, dims, jnp.float32)
    if shards:
        values = values * levels(key, dims, shards, -0.22, 0.18)
    return jnp.clip(values, -most, most).astype(held_as)


def setup_inputs(seed: int = 0, part: int = 0) -> dict:
    keys = jax.random.split(jax.random.key(seed), 8)
    part_keys = jax.random.split(jax.random.fold_in(keys[7], part), 8)
    queries = draw_queries(jax.random.fold_in(jax.random.fold_in(keys[7], part), 71), part)
    question_keys = normal_values(part_keys[1], (QT, KVH * HD), 1.0, 4.0, ((0, 128),))
    question_values = normal_values(part_keys[2], (QT, KVH * HD), 1.0, 5.0, ((0, 128),))
    doc_keys = draw_doc_keys(jax.random.fold_in(jax.random.fold_in(keys[7], part), 71), part)
    doc_values = normal_values(part_keys[4], (DOC, KVH * HD), 1.0, 5.0, ((0, 128),))
    lengths = jax.random.randint(part_keys[5], (NQ,), 4, QL + 1).astype(jnp.int32)
    offsets = draw_offsets(jax.random.fold_in(jax.random.fold_in(keys[7], part), 71), part)
    return {"queries": queries, "question_keys": question_keys, "question_values": question_values, "doc_keys": doc_keys, "doc_values": doc_values, "lengths": lengths, "offsets": offsets}


MASKED = -1.0e30


def row_tables(start, count, lengths, offsets):
    rows = start + jnp.arange(count, dtype=jnp.int32)
    question = rows // QL
    position = rows % QL
    owner_table = question[:, None] == jnp.arange(NQ, dtype=jnp.int32)[None, :]
    row_length = jnp.sum(jnp.where(owner_table, lengths[None, :], 0), axis=1)
    row_offset = jnp.sum(jnp.where(owner_table, offsets[None, :], 0), axis=1)
    return question, position, position < row_length, row_offset


def rounded(values):
    narrow = lax.optimization_barrier(values.astype(jnp.bfloat16))
    return narrow.astype(jnp.float32)


def reference(queries, question_keys, question_values, doc_keys, doc_values, lengths, offsets):
    total_rows = NQ * QL
    rows_block = total_rows // N_SEQ
    per_group = H // KVH
    factor_q = QSCALE ** -0.5
    question, position, live_rows, row_offset = row_tables(0, total_rows, lengths, offsets)
    query_all = queries.astype(jnp.float32).reshape(total_rows, KVH, per_group, HD)

    def visit(state, block):
        row_top, numer, denom = state
        doc_start = (block * DOC_DEV).astype(jnp.int32)
        self_start = (block * rows_block).astype(jnp.int32)
        key_doc = lax.dynamic_slice_in_dim(doc_keys, doc_start, DOC_DEV, 0).astype(jnp.float32).reshape(DOC_DEV, KVH, HD)
        value_doc = lax.dynamic_slice_in_dim(doc_values, doc_start, DOC_DEV, 0).astype(jnp.float32).reshape(DOC_DEV, KVH, HD)
        key_self = lax.dynamic_slice_in_dim(question_keys, self_start, rows_block, 0).astype(jnp.float32).reshape(rows_block, KVH, HD)
        value_self = lax.dynamic_slice_in_dim(question_values, self_start, rows_block, 0).astype(jnp.float32).reshape(rows_block, KVH, HD)
        doc_places = doc_start + jnp.arange(DOC_DEV, dtype=jnp.int32)
        self_rows = self_start + jnp.arange(rows_block, dtype=jnp.int32)
        mask_doc = live_rows[:, None] & (doc_places[None, :] < row_offset[:, None])
        mask_self = live_rows[:, None] & (self_rows[None, :] // QL == question[:, None]) & (self_rows[None, :] % QL <= position[:, None])
        mask_doc = mask_doc[:, None, None, :]
        mask_self = mask_self[:, None, None, :]
        scores_doc = jnp.einsum("rgjd,kgd->rgjk", query_all, key_doc) * factor_q
        scores_self = jnp.einsum("rgjd,kgd->rgjk", query_all, key_self) * factor_q
        scores_doc = jnp.where(mask_doc, scores_doc, MASKED)
        scores_self = jnp.where(mask_self, scores_self, MASKED)
        block_top = jnp.maximum(jnp.max(scores_doc, axis=-1), jnp.max(scores_self, axis=-1))
        weights_doc = rounded(jnp.where(mask_doc, jnp.exp(scores_doc - block_top[..., None]), 0.0))
        weights_self = rounded(jnp.where(mask_self, jnp.exp(scores_self - block_top[..., None]), 0.0))
        block_num = jnp.einsum("rgjk,kgd->rgjd", weights_doc, value_doc) + jnp.einsum("rgjk,kgd->rgjd", weights_self, value_self)
        block_den = jnp.sum(weights_doc, axis=-1) + jnp.sum(weights_self, axis=-1)
        new_top = jnp.maximum(row_top, block_top)
        old_factor = jnp.exp(row_top - new_top)
        new_factor = jnp.exp(block_top - new_top)
        numer = numer * old_factor[..., None] + block_num * new_factor[..., None]
        denom = denom * old_factor + block_den * new_factor
        return (new_top, numer, denom), None

    start_state = (jnp.full((total_rows, KVH, per_group), MASKED, jnp.float32),
                   jnp.zeros((total_rows, KVH, per_group, HD), jnp.float32),
                   jnp.zeros((total_rows, KVH, per_group), jnp.float32))
    final_state, unused = lax.scan(visit, start_state, jnp.arange(N_SEQ, dtype=jnp.int32))
    row_top, numer, denom = final_state
    safe_den = jnp.where(live_rows[:, None, None], denom, 1.0)
    result = numer / safe_den[..., None]
    result = jnp.where(live_rows[:, None, None, None], result, 0.0)
    return result.reshape(total_rows, H * HD).astype(jnp.bfloat16)
```

```python
import functools
import math

import jax
import jax.numpy as jnp
from jax import lax
from jax.experimental import pallas as pl
from jax.experimental.pallas import tpu as pltpu
from jax.sharding import PartitionSpec as P

H = 32
KVH = 16
HD = 128
QSCALE = 144
NEG = -1e30
HALF = H // 2
KVHALF = KVH // 2
GROUP = H // KVH
SCALE = QSCALE ** (-0.5) * math.log2(math.e)
CHUNKS = 4
ROW_TILES = 24

f32 = jnp.float32
bf16 = jnp.bfloat16


def kernel(
    nb,
    q_hbm, kq_hbm, vq_hbm, k_hbm, v_hbm, len_hbm, off_hbm,
    out_ref,
    q_in, kq_in, vq_in, len_s, off_s, rows32, send_rows, got_q, got_kv, turn32,
    mine_q, all_q, keys, vals, parts, stats, own_o, own_l, got_o, got_l, row_o, last,
    loc, ex_send, ex_recv, s1_send, s1_recv, s2_send, s2_recv,
    r1_send, r1_recv, st_recv, r2_send, r2_recv,
):
    rb = 2 * nb
    rows = rb * nb
    groups = max(rb // 8, 1)
    gs = rb // groups
    doc = k_hbm.shape[0]
    width = KVHALF * HD
    me = lax.axis_index("seq")
    c = lax.rem(me, 2)
    chip = me // 2
    x = lax.rem(chip, nb)
    y = chip // nb
    a = x * (1 - c) + y * c
    b = y * (1 - c) + x * c

    def dev(xx, yy, cc):
        return (yy * nb + xx) * 2 + cc

    def role_dev(aa, bb, cc):
        return dev(aa * (1 - c) + bb * c, bb * (1 - c) + aa * c, cc)

    def step(v, t):
        return lax.rem(v + t, nb)

    order = sorted(range(1, nb), key=lambda t: -min(t, nb - t))

    def send(src, dst, ssem, rsem, target):
        pltpu.make_async_remote_copy(
            src_ref=src, dst_ref=dst, send_sem=ssem, recv_sem=rsem,
            device_id={"seq": target}, device_id_type=pl.DeviceIdType.MESH,
        ).start()

    def await_bytes(ref, sem):
        pltpu.make_async_copy(ref, ref, sem).wait()

    mine = pl.ds(pl.multiple_of(c * width, 128), width)
    other = pl.ds(pl.multiple_of((1 - c) * width, 128), width)
    small = [
        pltpu.make_async_copy(q_hbm, q_in, loc.at[0]),
        pltpu.make_async_copy(kq_hbm, kq_in, loc.at[1]),
        pltpu.make_async_copy(vq_hbm, vq_in, loc.at[2]),
        pltpu.make_async_copy(len_hbm, len_s, loc.at[3]),
        pltpu.make_async_copy(off_hbm, off_s, loc.at[4]),
    ]
    large = [
        pltpu.make_async_copy(k_hbm.at[:, mine], keys.at[c], loc.at[5]),
        pltpu.make_async_copy(v_hbm.at[:, mine], vals.at[c], loc.at[6]),
    ]
    barrier = pltpu.get_barrier_semaphore()
    for t in range(1, nb):
        for cc in range(2):
            for target in (dev(step(x, t), y, cc), dev(x, step(y, t), cc)):
                pl.semaphore_signal(
                    barrier, inc=1, device_id={"seq": target},
                    device_id_type=pl.DeviceIdType.MESH,
                )
    pl.semaphore_signal(
        barrier, inc=1, device_id={"seq": dev(x, y, 1 - c)},
        device_id_type=pl.DeviceIdType.MESH,
    )
    for copy in small + large:
        copy.start()
    for copy in small:
        copy.wait()
    for h in range(H):
        rows32[h : h + 1, :] = q_in[:, h * HD : (h + 1) * HD].astype(f32)
    for g in range(KVH):
        rows32[H + g : H + g + 1, :] = kq_in[:, g * HD : (g + 1) * HD].astype(f32)
        rows32[H + KVH + g : H + KVH + g + 1, :] = vq_in[:, g * HD : (g + 1) * HD].astype(f32)
    for r in range(2):
        send_rows[r, 0] = rows32[r * HALF : (r + 1) * HALF, :].astype(bf16)
        at = H + r * KVHALF
        send_rows[r, 1] = jnp.concatenate(
            [rows32[at : at + KVHALF, :], rows32[at + KVH : at + KVH + KVHALF, :]], axis=0
        ).astype(bf16)
    got_q[b * 2 + c] = send_rows[c, 0]
    got_kv[a * 2 + c] = send_rows[c, 1]
    pl.semaphore_wait(barrier, 4 * (nb - 1) + 1)

    for t in order:
        send(send_rows.at[0, 0], got_q.at[y * 2 + c], s1_send, s1_recv.at[0], dev(x, step(y, t), 0))
        send(send_rows.at[1, 0], got_q.at[x * 2 + c], s1_send, s1_recv.at[0], dev(step(x, t), y, 1))
    send(send_rows.at[1 - c, 0], got_q.at[a * 2 + c], s1_send, s1_recv.at[0], dev(x, y, 1 - c))
    for t in order:
        send(send_rows.at[0, 1], got_kv.at[x * 2 + c], s1_send, s1_recv.at[1], dev(step(x, t), y, 0))
        send(send_rows.at[1, 1], got_kv.at[y * 2 + c], s1_send, s1_recv.at[1], dev(x, step(y, t), 1))
    send(send_rows.at[1 - c, 1], got_kv.at[b * 2 + c], s1_send, s1_recv.at[1], dev(x, y, 1 - c))
    send(k_hbm.at[:, other], keys.at[c], ex_send.at[0], ex_recv.at[0], dev(x, y, 1 - c))
    send(v_hbm.at[:, other], vals.at[c], ex_send.at[1], ex_recv.at[1], dev(x, y, 1 - c))

    await_bytes(got_q.at[0 : rb - 1], s1_recv.at[0])
    for i in range(rb):
        turn32[i * HALF : (i + 1) * HALF, :] = got_q[i].astype(f32)
    for h in range(HALF):
        block = turn32[pl.ds(h, rb, stride=HALF), :].astype(bf16)
        mine_q[h] = block
        all_q[h, pl.ds(pl.multiple_of(a * rb, rb), rb), :] = block

    per = HALF // CHUNKS
    for j in range(CHUNKS):
        for t in order:
            send(
                mine_q.at[pl.ds(j * per, per)],
                all_q.at[pl.ds(j * per, per), pl.ds(pl.multiple_of(a * rb, rb), rb), :],
                s2_send, s2_recv.at[j], role_dev(step(a, t), b, c),
            )

    await_bytes(got_kv.at[0 : rb - 1], s1_recv.at[1])
    for i in range(rb):
        turn32[i * HALF : (i + 1) * HALF, :] = got_kv[i].astype(f32)

    def row_of(aa, bb, cc):
        return dev(aa * (1 - c) + bb * c, bb * (1 - c) + aa * c, cc)

    spot = lax.rem(lax.broadcasted_iota(jnp.int32, (GROUP * rb, rb), 0), rb)
    key_spot = lax.broadcasted_iota(jnp.int32, (GROUP * rb, rb), 1)
    see = row_of(key_spot // 2, b, lax.rem(key_spot, 2)) <= row_of(a, spot // 2, lax.rem(spot, 2))
    lane = lax.broadcasted_iota(jnp.int32, (gs, 128), 1)
    own = jnp.full((gs, 128), NEG, f32)
    for g in range(KVHALF):
        key = turn32[pl.ds(g, rb, stride=HALF), :].astype(bf16)
        val = turn32[pl.ds(KVHALF + g, rb, stride=HALF), :].astype(bf16)
        q = mine_q[g * GROUP : (g + 1) * GROUP].reshape(GROUP * rb, HD)
        s = lax.dot_general(q, key, (((1,), (1,)), ((), ())), preferred_element_type=f32)
        s = jnp.where(see, s, NEG)
        top = jnp.max(s, axis=1, keepdims=True)
        p = jnp.exp2((s - top) * SCALE).astype(bf16)
        den = jnp.sum(p.astype(f32), axis=1, keepdims=True)
        num = jnp.dot(p, val, preferred_element_type=f32)
        own_o[g * GROUP : (g + 1) * GROUP] = (num / den).reshape(GROUP, rb, HD)
        level = top * SCALE + jnp.log2(den)
        for i in range(GROUP):
            for k in range(groups):
                at = i * rb + k * gs
                own = jnp.where(lane == k * HALF + g * GROUP + i, level[at : at + gs], own)
    own_l[...] = own

    for i in range(nb):
        stats[i] = jnp.full((gs, 128), NEG, f32)
    for copy in large:
        copy.wait()
    await_bytes(keys.at[1 - c], ex_recv.at[0])
    await_bytes(vals.at[1 - c], ex_recv.at[1])
    offset = off_s[0]
    places = lax.broadcasted_iota(jnp.int32, (1, doc), 1)
    seen = [places + (chip * 2 + blk) * doc < offset for blk in range(2)]
    ones = jnp.ones((doc, HD), bf16)

    def chunk(j, carry):
        first = j * per
        await_bytes(
            all_q.at[pl.ds(first, per), 0 : (nb - 1) * rb, :], s2_recv.at[j]
        )
        for u in range(per // GROUP):
            head = first + u * GROUP
            col = pl.ds(pl.multiple_of((head // GROUP) * HD, 128), HD)
            q = all_q[pl.ds(head, GROUP)].reshape(GROUP * rows, HD)
            tops, nums, dens = [], [], []
            for blk in range(2):
                s = lax.dot_general(
                    q, keys[blk, :, col], (((1,), (1,)), ((), ())), preferred_element_type=f32
                )
                s = jnp.where(seen[blk], s, NEG)
                top = jnp.max(s, axis=1, keepdims=True)
                p = jnp.exp2((s - top) * SCALE).astype(bf16)
                both = jnp.dot(
                    p, jnp.concatenate([vals[blk, :, col], ones], axis=1),
                    preferred_element_type=f32,
                )
                tops.append(top)
                nums.append(both[:, :HD])
                dens.append(both[:, HD:])
            top = jnp.maximum(tops[0], tops[1])
            w = [jnp.exp2((m - top) * SCALE) for m in tops]
            den = dens[0] * w[0] + dens[1] * w[1]
            inv = 1.0 / den
            o = nums[0] * (w[0] * inv) + nums[1] * (w[1] * inv)
            level = top * SCALE + jnp.log2(den)
            parts[pl.ds(head, GROUP)] = o.reshape(GROUP, rows, HD).astype(bf16)
            for i in range(nb):
                tile = stats[i]
                for z in range(GROUP):
                    for k in range(groups):
                        at = z * rows + i * rb + k * gs
                        tile = jnp.where(lane == k * HALF + head + z, level[at : at + gs], tile)
                stats[i] = tile
        for t in order:
            peer = step(a, t)
            send(
                parts.at[pl.ds(first, per), pl.ds(pl.multiple_of(peer * rb, rb), rb), :],
                got_o.at[a, pl.ds(first, per)],
                r1_send, r1_recv.at[j], role_dev(peer, b, c),
            )
        return carry

    lax.fori_loop(0, CHUNKS, chunk, 0)
    for t in order:
        peer = step(a, t)
        send(stats.at[peer], got_l.at[a], r1_send, st_recv, role_dev(peer, b, c))

    await_bytes(got_l.at[0 : nb - 1], st_recv)
    levels = [stats[a]] + [got_l[step(a, t)] for t in range(1, nb)] + [own_l[...]]
    top = functools.reduce(jnp.maximum, levels)
    weights = [jnp.exp2(v - top) for v in levels]
    total = functools.reduce(jnp.add, weights)
    inv = 1.0 / total
    weights = [w * inv for w in weights]
    level = top + jnp.log2(total)
    for j in range(CHUNKS):
        await_bytes(got_o.at[0 : nb - 1, pl.ds(j * per, per)], r1_recv.at[j])
        for h in range(j * per, (j + 1) * per):
            full = [parts[h, pl.ds(pl.multiple_of(a * rb, rb), rb), :].astype(f32)]
            full += [got_o[step(a, t), h].astype(f32) for t in range(1, nb)]
            full += [own_o[h]]
            for k in range(groups):
                at = k * HALF + h
                acc = weights[0][:, at : at + 1] * full[0][k * gs : (k + 1) * gs]
                for w, part in zip(weights[1:], full[1:]):
                    acc += w[:, at : at + 1] * part[k * gs : (k + 1) * gs]
                row_o[pl.ds(k * gs * ROW_TILES + h, gs, stride=ROW_TILES), :] = acc
    for h in range(HALF // 2):
        for k in range(groups):
            at = k * HALF + h
            pair = jnp.where(
                lane < 64, level[:, at : at + 1], level[:, at + HALF // 2 : at + HALF // 2 + 1]
            )
            row_o[pl.ds(k * gs * ROW_TILES + HALF + h, gs, stride=ROW_TILES), :] = pair

    def row_at(i):
        return pl.ds(pl.multiple_of(i * ROW_TILES, 8), ROW_TILES)

    for t in order:
        peer = step(b, t)
        for cc in range(2):
            send(
                row_o.at[row_at(peer * 2 + cc)], last.at[c * nb + b],
                r2_send, r2_recv, role_dev(a, peer, cc),
            )
    send(
        row_o.at[row_at(b * 2 + 1 - c)], last.at[c * nb + b],
        r2_send, r2_recv, dev(x, y, 1 - c),
    )
    last[c * nb + b] = row_o[row_at(b * 2 + c), :]
    await_bytes(last.at[0 : 2 * nb - 1], r2_recv)

    live = jnp.full((HALF // 2, 128), me, jnp.int32) < len_s[0]
    for r in range(2):
        levels = [last[r * nb + i, HALF:, :] for i in range(nb)]
        top = functools.reduce(jnp.maximum, levels)
        weights = [jnp.exp2(v - top) for v in levels]
        inv = 1.0 / functools.reduce(jnp.add, weights)
        outs = []
        for k in range(2):
            acc = None
            for i in range(nb):
                w = weights[i] * inv
                term = w[:, k * 64 : k * 64 + 1] * last[
                    r * nb + i, k * HALF // 2 : (k + 1) * HALF // 2, :
                ]
                acc = term if acc is None else acc + term
            outs.append(jnp.where(live, acc, 0.0))
        out_ref[r * HALF : (r + 1) * HALF, :] = jnp.concatenate(outs, axis=0).astype(bf16)

    await_bytes(got_q.at[0 : rb - 1], s1_send)
    await_bytes(got_kv.at[0 : rb - 1], s1_send)
    for i, buf in enumerate((keys, vals)):
        await_bytes(buf.at[c], ex_send.at[i])
    await_bytes(all_q.at[:, 0 : (nb - 1) * rb, :], s2_send)
    await_bytes(got_o.at[0 : nb - 1], r1_send)
    await_bytes(got_l.at[0 : nb - 1], r1_send)
    await_bytes(last.at[0 : 2 * nb - 1], r2_send)


def local(nb, q, kq, vq, k, v, lengths, offsets):
    rb = 2 * nb
    rows = rb * nb
    doc = k.shape[0]
    gs = rb // max(rb // 8, 1)
    dma = pltpu.SemaphoreType.DMA
    out = pl.pallas_call(
        functools.partial(kernel, nb),
        out_shape=jax.ShapeDtypeStruct((H, HD), bf16),
        in_specs=[pl.BlockSpec(memory_space=pl.ANY)] * 7,
        out_specs=pl.BlockSpec(memory_space=pltpu.VMEM),
        scratch_shapes=[
            pltpu.VMEM((1, H * HD), bf16),
            pltpu.VMEM((1, KVH * HD), bf16),
            pltpu.VMEM((1, KVH * HD), bf16),
            pltpu.SMEM((1,), jnp.int32),
            pltpu.SMEM((1,), jnp.int32),
            pltpu.VMEM((H + 2 * KVH, HD), f32),
            pltpu.VMEM((2, 2, HALF, HD), bf16),
            pltpu.VMEM((rb, HALF, HD), bf16),
            pltpu.VMEM((rb, HALF, HD), bf16),
            pltpu.VMEM((rb * HALF, HD), f32),
            pltpu.VMEM((HALF, rb, HD), bf16),
            pltpu.VMEM((HALF, rows, HD), bf16),
            pltpu.VMEM((2, doc, KVHALF * HD), bf16),
            pltpu.VMEM((2, doc, KVHALF * HD), bf16),
            pltpu.VMEM((HALF, rows, HD), bf16),
            pltpu.VMEM((nb, gs, 128), f32),
            pltpu.VMEM((HALF, rb, HD), f32),
            pltpu.VMEM((gs, 128), f32),
            pltpu.VMEM((nb, HALF, rb, HD), bf16),
            pltpu.VMEM((nb, gs, 128), f32),
            pltpu.VMEM((rb * ROW_TILES, HD), f32),
            pltpu.VMEM((2 * nb, ROW_TILES, HD), f32),
            dma((7,)), dma((2,)), dma((2,)), dma, dma((2,)), dma, dma((CHUNKS,)),
            dma, dma((CHUNKS,)), dma, dma, dma,
        ],
        compiler_params=pltpu.CompilerParams(
            collective_id=0, has_side_effects=True, vmem_limit_bytes=56 * 1024 * 1024
        ),
    )(q, kq, vq, k, v, lengths, offsets)
    return out.reshape(1, H * HD)


def solution(mesh):
    nb = math.isqrt(mesh.shape["seq"] // 2)
    rows = P(("grp", "seq"), None)
    return jax.shard_map(
        functools.partial(local, nb),
        mesh=mesh,
        in_specs=(rows, rows, rows, rows, rows, P("grp"), P("grp")),
        out_specs=rows,
        check_vma=False,
    )
```

```python
import functools
import math

import jax
import jax.numpy as jnp
from jax import lax
from jax.experimental import pallas as pl
from jax.experimental.pallas import tpu as pltpu
from jax.sharding import PartitionSpec as P

H = 32
KVH = 16
HD = 128
QSCALE = 144
NEG = -1e30
HALF = H // 2
KVHALF = KVH // 2
GROUP = H // KVH
SCALE = QSCALE ** (-0.5) * math.log2(math.e)
CHUNKS = 4
ROW_TILES = 24

f32 = jnp.float32
bf16 = jnp.bfloat16


def kernel(
    nb,
    q_hbm, kq_hbm, vq_hbm, k_hbm, v_hbm, len_hbm, off_hbm,
    out_ref,
    q_in, kq_in, vq_in, len_s, off_s, rows32, send_rows, got_q, got_kv, turn32,
    mine_q, all_q, keys, vals, parts, stats, own_o, own_l, got_o, got_l, row_o, last,
    spare_q, first_q, first_o, first_l, pair_k, pair_v,
    loc, ex_send, ex_recv, s1_send, s1_recv, s2_send, s2_recv,
    r1_send, r1_recv, st_recv, r2_send, r2_recv,
    here, spare_recv, relay_recv, relay_send, first_send, first_recv, back_send, back_recv,
):
    rb = 2 * nb
    rows = rb * nb
    groups = max(rb // 8, 1)
    gs = rb // groups
    doc = k_hbm.shape[0]
    width = KVHALF * HD
    me = lax.axis_index("seq")
    c = lax.rem(me, 2)
    chip = me // 2
    x = lax.rem(chip, nb)
    y = chip // nb
    a = x * (1 - c) + y * c
    b = y * (1 - c) + x * c

    def dev(xx, yy, cc):
        return (yy * nb + xx) * 2 + cc

    def role_dev(aa, bb, cc):
        return dev(aa * (1 - c) + bb * c, bb * (1 - c) + aa * c, cc)

    def step(v, t):
        return lax.rem(v + t, nb)

    zero = me == 0
    rest = me > 0
    stand = dev(0, 1, 0)
    order = sorted(range(1, nb), key=lambda t: -min(t, nb - t))

    def send(src, dst, ssem, rsem, target):
        pltpu.make_async_remote_copy(
            src_ref=src, dst_ref=dst, send_sem=ssem, recv_sem=rsem,
            device_id={"seq": target}, device_id_type=pl.DeviceIdType.MESH,
        ).start()

    def await_bytes(ref, sem):
        pltpu.make_async_copy(ref, ref, sem).wait()

    mine = pl.ds(pl.multiple_of(c * width, 128), width)
    other = pl.ds(pl.multiple_of((1 - c) * width, 128), width)
    small = [
        pltpu.make_async_copy(q_hbm, q_in, loc.at[0]),
        pltpu.make_async_copy(kq_hbm, kq_in, loc.at[1]),
        pltpu.make_async_copy(vq_hbm, vq_in, loc.at[2]),
        pltpu.make_async_copy(len_hbm, len_s, loc.at[3]),
        pltpu.make_async_copy(off_hbm, off_s, loc.at[4]),
    ]
    large = [
        pltpu.make_async_copy(k_hbm.at[:, mine], keys.at[c], loc.at[5]),
        pltpu.make_async_copy(v_hbm.at[:, mine], vals.at[c], loc.at[6]),
    ]
    for copy in small + large:
        copy.start()
    mate = dev(x, y, 1 - c)

    def send_keys():
        send(k_hbm.at[:, other], keys.at[c], ex_send.at[0], ex_recv.at[0], mate)
        send(v_hbm.at[:, other], vals.at[c], ex_send.at[1], ex_recv.at[1], mate)

    barrier = pltpu.get_barrier_semaphore()

    def signal(sem, target):
        pl.semaphore_signal(
            sem, inc=1, device_id={"seq": target}, device_id_type=pl.DeviceIdType.MESH
        )

    @pl.when(rest)
    def _():
        for t in order:
            for cc in range(2):
                signal(barrier, dev(step(x, t), y, cc))
                signal(barrier, dev(x, step(y, t), cc))
        signal(barrier, dev(x, y, 1 - c))

    @pl.when((x > 0) & (y > 0))
    def _():
        signal(barrier, 0)

    for copy in small:
        copy.wait()
    for h in range(H):
        rows32[h : h + 1, :] = q_in[:, h * HD : (h + 1) * HD].astype(f32)
    for g in range(KVH):
        rows32[H + g : H + g + 1, :] = kq_in[:, g * HD : (g + 1) * HD].astype(f32)
        rows32[H + KVH + g : H + KVH + g + 1, :] = vq_in[:, g * HD : (g + 1) * HD].astype(f32)
    for r in range(2):
        send_rows[r, 0] = rows32[r * HALF : (r + 1) * HALF, :].astype(bf16)
        at = H + r * KVHALF
        send_rows[r, 1] = jnp.concatenate(
            [rows32[at : at + KVHALF, :], rows32[at + KVH : at + KVH + KVHALF, :]], axis=0
        ).astype(bf16)
    got_kv[a * 2 + c] = send_rows[c, 1]

    @pl.when(rest)
    def _():
        got_q[b * 2 + c] = send_rows[c, 0]

    @pl.when(a == 0)
    def _():
        got_q[0] = jnp.zeros((HALF, HD), bf16)

    line = 4 * (nb - 1) + 1
    near = jnp.where((x == 0) | (y == 0), 1, 0)
    pl.semaphore_wait(barrier, jnp.where(zero, 2 * nb * nb - 1, line - near))

    @pl.when(zero)
    def _():
        signal(here, 1)
        for t in order:
            for cc in range(2):
                signal(here, dev(t, 0, cc))
        send_keys()
        first_q[...] = send_rows[0, 0]
        far = sorted(
            ((xx, yy) for xx in range(nb) for yy in range(nb)),
            key=lambda p: -min(p[0], nb - p[0]) - min(p[1], nb - p[1]),
        )
        for xx, yy in far:
            for cc in range(2):
                if xx or yy or cc:
                    send(send_rows.at[cc, 0], first_q, first_send, first_recv, dev(xx, yy, cc))

    my_block = pl.ds(pl.multiple_of(a * rb, rb), rb)
    per = HALF // CHUNKS

    def send_mate_row(k, slot):
        send(send_rows.at[1 - c, k], slot, s1_send.at[k], s1_recv.at[k], mate)

    @pl.when(rest)
    def _():
        for t in order:
            to_0 = dev(x, step(y, t), 0)

            @pl.when(to_0 > 0)
            def _(to_0=to_0):
                send(send_rows.at[0, 0], got_q.at[y * 2 + c], s1_send.at[0], s1_recv.at[0], to_0)

            send(
                send_rows.at[1, 0], got_q.at[x * 2 + c], s1_send.at[0], s1_recv.at[0],
                dev(step(x, t), y, 1),
            )

        @pl.when(me > 1)
        def _():
            send_mate_row(0, got_q.at[a * 2 + c])

    def send_row_0(target):
        send(send_rows.at[0, 1], got_kv.at[x * 2 + c], s1_send.at[1], s1_recv.at[1], target)

    for t in order:
        to_0 = dev(step(x, t), y, 0)

        @pl.when(to_0 > 0)
        def _(to_0=to_0):
            send_row_0(to_0)

        send(
            send_rows.at[1, 1], got_kv.at[y * 2 + c], s1_send.at[1], s1_recv.at[1],
            dev(x, step(y, t), 1),
        )

    @pl.when(me != 1)
    def _():
        send_mate_row(1, got_kv.at[b * 2 + c])

    @pl.when(me > 1)
    def _():
        send_keys()

    @pl.when(rest)
    def _():
        @pl.when(a == 0)
        def _():
            await_bytes(got_q.at[0 : rb - 2], s1_recv.at[0])

        @pl.when(a > 0)
        def _():
            await_bytes(got_q.at[0 : rb - 1], s1_recv.at[0])

        for i in range(rb):
            turn32[i * HALF : (i + 1) * HALF, :] = got_q[i].astype(f32)
        for h in range(HALF):
            block = turn32[pl.ds(h, rb, stride=HALF), :].astype(bf16)
            mine_q[h] = block
            all_q[h, my_block, :] = block
        for j in range(CHUNKS):
            some = pl.ds(j * per, per)

            @pl.when(me == stand)
            def _(some=some, j=j):
                send(
                    mine_q.at[some], spare_q.at[some, my_block, :],
                    relay_send.at[0], relay_recv.at[j], 1,
                )

            for t in order:
                target = role_dev(step(a, t), b, c)

                @pl.when(target > 0)
                def _(some=some, target=target, j=j):
                    send(
                        mine_q.at[some], all_q.at[some, my_block, :],
                        s2_send, s2_recv.at[j], target,
                    )

                @pl.when(target == 0)
                def _(some=some, j=j):
                    send(
                        mine_q.at[some], spare_q.at[some, my_block, :],
                        s2_send, spare_recv.at[j], 1,
                    )

    @pl.when((y == 0) & rest)
    def _():
        pl.semaphore_wait(here, 1)

        @pl.when(me == 1)
        def _():
            send_keys()
            send_mate_row(1, got_kv.at[b * 2 + c])
            for j in range(CHUNKS):
                block = spare_q.at[pl.ds(j * per, per), 0:rb, :]
                await_bytes(block, relay_recv.at[j])
                for t in order:
                    send(
                        block, all_q.at[pl.ds(j * per, per), 0:rb, :],
                        relay_send.at[1], s2_recv.at[j], dev(t, 0, 0),
                    )

        @pl.when(me > 1)
        def _():
            send_row_0(0)

    lane = lax.broadcasted_iota(jnp.int32, (gs, 128), 1)
    for i in range(nb):
        stats[i] = jnp.full((gs, 128), NEG, f32)
    for copy in large:
        copy.wait()
    await_bytes(keys.at[1 - c], ex_recv.at[0])
    await_bytes(vals.at[1 - c], ex_recv.at[1])
    offset = off_s[0]
    places = lax.broadcasted_iota(jnp.int32, (1, doc), 1)
    seen = [places + (chip * 2 + blk) * doc < offset for blk in range(2)]
    ones = jnp.ones((doc, HD), bf16)

    def chunk(j, carry):
        first = j * per

        @pl.when(me == 1)
        def _():
            some = pl.ds(first, per)
            await_bytes(spare_q.at[some, rb:, :], spare_recv.at[j])
            send(spare_q.at[some], all_q.at[some], relay_send.at[2], s2_recv.at[j], 0)

        @pl.when(zero)
        def _():
            await_bytes(all_q.at[pl.ds(first, per)], s2_recv.at[j])

        @pl.when(rest)
        def _():
            await_bytes(all_q.at[pl.ds(first, per), 0 : (nb - 1) * rb, :], s2_recv.at[j])

        for u in range(per // GROUP):
            head = first + u * GROUP
            col = pl.ds(pl.multiple_of((head // GROUP) * HD, 128), HD)
            q = all_q[pl.ds(head, GROUP)].reshape(GROUP * rows, HD)
            tops, nums, dens = [], [], []
            for blk in range(2):
                s = lax.dot_general(
                    q, keys[blk, :, col], (((1,), (1,)), ((), ())), preferred_element_type=f32
                )
                s = jnp.where(seen[blk], s, NEG)
                top = jnp.max(s, axis=1, keepdims=True)
                p = jnp.exp2((s - top) * SCALE).astype(bf16)
                both = jnp.dot(
                    p, jnp.concatenate([vals[blk, :, col], ones], axis=1),
                    preferred_element_type=f32,
                )
                tops.append(top)
                nums.append(both[:, :HD])
                dens.append(both[:, HD:])
            top = jnp.maximum(tops[0], tops[1])
            w = [jnp.exp2((m - top) * SCALE) for m in tops]
            den = dens[0] * w[0] + dens[1] * w[1]
            inv = 1.0 / den
            o = nums[0] * (w[0] * inv) + nums[1] * (w[1] * inv)
            level = top * SCALE + jnp.log2(den)
            parts[pl.ds(head, GROUP)] = o.reshape(GROUP, rows, HD).astype(bf16)
            for i in range(nb):
                tile = stats[i]
                for z in range(GROUP):
                    for k in range(groups):
                        at = z * rows + i * rb + k * gs
                        tile = jnp.where(lane == k * HALF + head + z, level[at : at + gs], tile)
                stats[i] = tile
        for t in order:
            peer = step(a, t)
            send(
                parts.at[pl.ds(first, per), pl.ds(pl.multiple_of(peer * rb, rb), rb), :],
                got_o.at[a, pl.ds(first, per)],
                r1_send.at[0], r1_recv.at[j], role_dev(peer, b, c),
            )
        return carry

    lax.fori_loop(0, CHUNKS, chunk, 0)
    for t in order:
        peer = step(a, t)
        send(stats.at[peer], got_l.at[a], r1_send.at[1], st_recv, role_dev(peer, b, c))

    await_bytes(got_kv.at[0 : rb - 1], s1_recv.at[1])
    for i in range(rb):
        turn32[i * HALF : (i + 1) * HALF, :] = got_kv[i].astype(f32)

    def row_of(aa, bb, cc):
        return dev(aa * (1 - c) + bb * c, bb * (1 - c) + aa * c, cc)

    spot = lax.rem(lax.broadcasted_iota(jnp.int32, (GROUP * rb, rb), 0), rb)
    key_spot = lax.broadcasted_iota(jnp.int32, (GROUP * rb, rb), 1)
    see = row_of(key_spot // 2, b, lax.rem(key_spot, 2)) <= row_of(a, spot // 2, lax.rem(spot, 2))
    own = jnp.full((gs, 128), NEG, f32)
    for g in range(KVHALF):
        key = turn32[pl.ds(g, rb, stride=HALF), :].astype(bf16)
        val = turn32[pl.ds(KVHALF + g, rb, stride=HALF), :].astype(bf16)
        q = all_q[g * GROUP : (g + 1) * GROUP, my_block, :].reshape(GROUP * rb, HD)
        s = lax.dot_general(q, key, (((1,), (1,)), ((), ())), preferred_element_type=f32)
        s = jnp.where(see, s, NEG)
        top = jnp.max(s, axis=1, keepdims=True)
        p = jnp.exp2((s - top) * SCALE).astype(bf16)
        den = jnp.sum(p.astype(f32), axis=1, keepdims=True)
        num = jnp.dot(p, val, preferred_element_type=f32)
        own_o[g * GROUP : (g + 1) * GROUP] = (num / den).reshape(GROUP, rb, HD)
        level = top * SCALE + jnp.log2(den)
        for i in range(GROUP):
            for k in range(groups):
                at = i * rb + k * gs
                own = jnp.where(lane == k * HALF + g * GROUP + i, level[at : at + gs], own)
    own_l[...] = own

    @pl.when(rest)
    def _():
        await_bytes(first_q, first_recv)

    head_of = lax.broadcasted_iota(jnp.int32, (HALF, HD), 0) // GROUP
    wide = jnp.concatenate(
        [jnp.where(head_of == g, first_q[...], jnp.zeros((), bf16)) for g in range(KVHALF)], axis=1
    )
    tops, nums, dens = [], [], []
    for blk in range(2):
        s = lax.dot_general(
            wide, keys[blk], (((1,), (1,)), ((), ())), preferred_element_type=f32
        )
        s = jnp.where(seen[blk], s, NEG)
        top = jnp.max(s, axis=1, keepdims=True)
        p = jnp.exp2((s - top) * SCALE).astype(bf16)
        dens.append(jnp.sum(p.astype(f32), axis=1, keepdims=True))
        num = jnp.dot(p, vals[blk], preferred_element_type=f32)
        pick = jnp.zeros((HALF, HD), f32)
        for g in range(KVHALF):
            pick = jnp.where(head_of == g, num[:, g * HD : (g + 1) * HD], pick)
        tops.append(top)
        nums.append(pick)
    top = jnp.maximum(tops[0], tops[1])
    w = [jnp.exp2((m - top) * SCALE) for m in tops]
    den = dens[0] * w[0] + dens[1] * w[1]
    level = top * SCALE + jnp.log2(den)
    half_lane = lax.broadcasted_iota(jnp.int32, (HALF // 2, 128), 1) < 64

    def paired(v):
        return jnp.where(half_lane, v[: HALF // 2], v[HALF // 2 :])

    first_o[a] = ((nums[0] * w[0] + nums[1] * w[1]) / den).astype(bf16)
    first_l[a] = paired(level)

    @pl.when(a > 0)
    def _():
        target = role_dev(0, b, c)
        send(first_o.at[a], first_o.at[a], back_send.at[0], back_recv.at[0], target)
        send(first_l.at[a], first_l.at[a], back_send.at[1], back_recv.at[1], target)

    await_bytes(got_l.at[0 : nb - 1], st_recv)
    levels = [stats[a]] + [got_l[step(a, t)] for t in range(1, nb)] + [own_l[...]]
    top = functools.reduce(jnp.maximum, levels)
    weights = [jnp.exp2(v - top) for v in levels]
    total = functools.reduce(jnp.add, weights)
    inv = 1.0 / total
    weights = [w * inv for w in weights]
    level = top + jnp.log2(total)
    for j in range(CHUNKS):
        await_bytes(got_o.at[0 : nb - 1, pl.ds(j * per, per)], r1_recv.at[j])
        for h in range(j * per, (j + 1) * per):
            full = [parts[h, pl.ds(pl.multiple_of(a * rb, rb), rb), :].astype(f32)]
            full += [got_o[step(a, t), h].astype(f32) for t in range(1, nb)]
            full += [own_o[h]]
            for k in range(groups):
                at = k * HALF + h
                acc = weights[0][:, at : at + 1] * full[0][k * gs : (k + 1) * gs]
                for w, part in zip(weights[1:], full[1:]):
                    acc += w[:, at : at + 1] * part[k * gs : (k + 1) * gs]
                row_o[pl.ds(k * gs * ROW_TILES + h, gs, stride=ROW_TILES), :] = acc
    for h in range(HALF // 2):
        for k in range(groups):
            at = k * HALF + h
            pair = jnp.where(
                lane < 64, level[:, at : at + 1], level[:, at + HALF // 2 : at + HALF // 2 + 1]
            )
            row_o[pl.ds(k * gs * ROW_TILES + HALF + h, gs, stride=ROW_TILES), :] = pair

    def row_at(i):
        return pl.ds(pl.multiple_of(i * ROW_TILES, 8), ROW_TILES)

    def spread(w, k):
        return w[:, k * 64 : k * 64 + 1]

    def merged(levels, values):
        top = functools.reduce(jnp.maximum, levels)
        weights = [jnp.exp2(v - top) for v in levels]
        total = functools.reduce(jnp.add, weights)
        inv = 1.0 / total
        outs = []
        for k in range(2):
            terms = [
                spread(w * inv, k) * v[k * HALF // 2 : (k + 1) * HALF // 2]
                for w, v in zip(weights, values)
            ]
            outs.append(functools.reduce(jnp.add, terms))
        return jnp.concatenate(outs, axis=0), top + jnp.log2(total)

    @pl.when(a == 0)
    def _():
        await_bytes(first_o.at[0 : nb - 1], back_recv.at[0])
        await_bytes(first_l.at[0 : nb - 1], back_recv.at[1])
        pair = got_kv[0].astype(f32)
        for i in range(GROUP):
            pair_k[pl.ds(i, KVHALF, stride=GROUP), :] = pair[:KVHALF]
            pair_v[pl.ds(i, KVHALF, stride=GROUP), :] = pair[KVHALF:]
        score = jnp.sum(first_q[...].astype(f32) * pair_k[...], axis=1, keepdims=True) * SCALE
        score = jnp.where(jnp.full((HALF // 2, 128), b, jnp.int32) == 0, paired(score), NEG)
        values, level = merged(
            [first_l[i] for i in range(nb)] + [score],
            [first_o[i].astype(f32) for i in range(nb)] + [pair_v[...]],
        )
        row_o[0:HALF, :] = values
        row_o[HALF:ROW_TILES, :] = level

    for t in order:
        peer = step(b, t)
        for cc in range(2):
            send(
                row_o.at[row_at(peer * 2 + cc)], last.at[c * nb + b],
                r2_send, r2_recv, role_dev(a, peer, cc),
            )
    send(row_o.at[row_at(b * 2 + 1 - c)], last.at[c * nb + b], r2_send, r2_recv, mate)
    last[c * nb + b] = row_o[row_at(b * 2 + c), :]
    await_bytes(last.at[0 : 2 * nb - 1], r2_recv)

    live = jnp.full((HALF, 128), me, jnp.int32) < len_s[0]
    for r in range(2):
        got = [last[r * nb + i] for i in range(nb)]
        values, _ = merged([v[HALF:] for v in got], [v[:HALF] for v in got])
        out_ref[r * HALF : (r + 1) * HALF, :] = jnp.where(live, values, 0.0).astype(bf16)

    @pl.when(rest & (x == 0))
    def _():
        await_bytes(got_q.at[0 : rb - 2], s1_send.at[0])

    @pl.when(x > 0)
    def _():
        await_bytes(got_q.at[0 : rb - 1], s1_send.at[0])

    await_bytes(got_kv.at[0 : rb - 1], s1_send.at[1])
    for i, buf in enumerate((keys, vals)):
        await_bytes(buf.at[c], ex_send.at[i])
    await_bytes(got_o.at[0 : nb - 1], r1_send.at[0])
    await_bytes(got_l.at[0 : nb - 1], r1_send.at[1])

    @pl.when(rest)
    def _():
        await_bytes(all_q.at[:, 0 : (nb - 1) * rb, :], s2_send)

    @pl.when(a > 0)
    def _():
        await_bytes(first_o.at[a], back_send.at[0])
        await_bytes(first_l.at[a], back_send.at[1])

    @pl.when(me == stand)
    def _():
        await_bytes(mine_q, relay_send.at[0])

    @pl.when(me == 1)
    def _():
        await_bytes(all_q.at[:, rb:, :], relay_send.at[1])
        await_bytes(all_q, relay_send.at[2])

    await_bytes(last.at[0 : 2 * nb - 1], r2_send)

    @pl.when(zero)
    def _():
        await_bytes(got_o.at[0 : nb - 1, :, 0:rb, :], first_send)
        await_bytes(got_q.at[0 : rb - 1], first_send)


def local(nb, q, kq, vq, k, v, lengths, offsets):
    rb = 2 * nb
    rows = rb * nb
    doc = k.shape[0]
    gs = rb // max(rb // 8, 1)
    dma = pltpu.SemaphoreType.DMA
    out = pl.pallas_call(
        functools.partial(kernel, nb),
        out_shape=pltpu.VMEM((H, HD), bf16),
        in_specs=[pl.BlockSpec(memory_space=pltpu.HBM)] * 7,
        out_specs=pl.BlockSpec(memory_space=pltpu.VMEM),
        scratch_shapes=[
            pltpu.VMEM((1, H * HD), bf16),
            pltpu.VMEM((1, KVH * HD), bf16),
            pltpu.VMEM((1, KVH * HD), bf16),
            pltpu.SMEM((1,), jnp.int32),
            pltpu.SMEM((1,), jnp.int32),
            pltpu.VMEM((H + 2 * KVH, HD), f32),
            pltpu.VMEM((2, 2, HALF, HD), bf16),
            pltpu.VMEM((rb, HALF, HD), bf16),
            pltpu.VMEM((rb, HALF, HD), bf16),
            pltpu.VMEM((rb * HALF, HD), f32),
            pltpu.VMEM((HALF, rb, HD), bf16),
            pltpu.VMEM((HALF, rows, HD), bf16),
            pltpu.VMEM((2, doc, KVHALF * HD), bf16),
            pltpu.VMEM((2, doc, KVHALF * HD), bf16),
            pltpu.VMEM((HALF, rows, HD), bf16),
            pltpu.VMEM((nb, gs, 128), f32),
            pltpu.VMEM((HALF, rb, HD), f32),
            pltpu.VMEM((gs, 128), f32),
            pltpu.VMEM((nb, HALF, rb, HD), bf16),
            pltpu.VMEM((nb, gs, 128), f32),
            pltpu.VMEM((rb * ROW_TILES, HD), f32),
            pltpu.VMEM((2 * nb, ROW_TILES, HD), f32),
            pltpu.VMEM((HALF, rows, HD), bf16),
            pltpu.VMEM((HALF, HD), bf16),
            pltpu.VMEM((nb, HALF, HD), bf16),
            pltpu.VMEM((nb, HALF // 2, HD), f32),
            pltpu.VMEM((HALF, HD), f32),
            pltpu.VMEM((HALF, HD), f32),
            dma((7,)), dma((2,)), dma((2,)), dma((2,)), dma((2,)), dma, dma((CHUNKS,)),
            dma((2,)), dma((CHUNKS,)), dma, dma, dma,
            pltpu.SemaphoreType.REGULAR, dma((CHUNKS,)), dma((CHUNKS,)), dma((3,)), dma, dma, dma((2,)), dma((2,)),
        ],
        compiler_params=pltpu.CompilerParams(
            collective_id=0, has_side_effects=True, vmem_limit_bytes=56 * 1024 * 1024
        ),
    )(q, kq, vq, k, v, lengths, offsets)
    return out.reshape(1, H * HD)


def solution(mesh):
    nb = math.isqrt(mesh.shape["seq"] // 2)
    rows = P(("grp", "seq"), None)
    return jax.shard_map(
        functools.partial(local, nb),
        mesh=mesh,
        in_specs=(rows, rows, rows, rows, rows, P("grp"), P("grp")),
        out_specs=rows,
        check_vma=False,
    )
```

```python
import functools
import math

import jax
import jax.numpy as jnp
from jax import lax
from jax.experimental import pallas as pl
from jax.experimental.pallas import tpu as pltpu
from jax.sharding import PartitionSpec as P

H = 32
KVH = 16
HD = 128
QSCALE = 144
NEG = -1e30
HALF = H // 2
KVHALF = KVH // 2
GROUP = H // KVH
SCALE = QSCALE ** (-0.5) * math.log2(math.e)
CHUNKS = 4
ROW_TILES = 24

f32 = jnp.float32
bf16 = jnp.bfloat16


def kernel(
    nb,
    q_hbm, kq_hbm, vq_hbm, k_hbm, v_hbm, len_hbm, off_hbm,
    out_ref,
    q_in, kq_in, vq_in, len_s, off_s, rows32, send_rows, got_q, got_kv, turn32,
    mine_q, all_q, keys, vals, parts, stats, own_o, own_l, got_o, got_l, row_o, last,
    mate_q, spare_q, first_q, first_o, first_l, pair_k, pair_v,
    loc, ex_send, ex_recv, s1_send, s1_recv, s2_send, s2_recv,
    r1_send, r1_recv, st_recv, r2_send, r2_recv,
    here, spare_recv, relay_recv, relay_send, first_send, first_recv, back_send, back_recv,
):
    rb = 2 * nb
    rows = rb * nb
    groups = max(rb // 8, 1)
    gs = rb // groups
    doc = k_hbm.shape[0]
    width = KVHALF * HD
    me = lax.axis_index("seq")
    c = lax.rem(me, 2)
    chip = me // 2
    x = lax.rem(chip, nb)
    y = chip // nb
    a = x * (1 - c) + y * c
    b = y * (1 - c) + x * c

    def dev(xx, yy, cc):
        return (yy * nb + xx) * 2 + cc

    def role_dev(aa, bb, cc):
        return dev(aa * (1 - c) + bb * c, bb * (1 - c) + aa * c, cc)

    def step(v, t):
        return lax.rem(v + t, nb)

    zero = me == 0
    rest = me > 0
    order = sorted(range(1, nb), key=lambda t: -min(t, nb - t))

    def send(src, dst, ssem, rsem, target):
        pltpu.make_async_remote_copy(
            src_ref=src, dst_ref=dst, send_sem=ssem, recv_sem=rsem,
            device_id={"seq": target}, device_id_type=pl.DeviceIdType.MESH,
        ).start()

    def await_bytes(ref, sem):
        pltpu.make_async_copy(ref, ref, sem).wait()

    mine = pl.ds(pl.multiple_of(c * width, 128), width)
    other = pl.ds(pl.multiple_of((1 - c) * width, 128), width)
    small = [
        pltpu.make_async_copy(q_hbm, q_in, loc.at[0]),
        pltpu.make_async_copy(kq_hbm, kq_in, loc.at[1]),
        pltpu.make_async_copy(vq_hbm, vq_in, loc.at[2]),
        pltpu.make_async_copy(len_hbm, len_s, loc.at[3]),
        pltpu.make_async_copy(off_hbm, off_s, loc.at[4]),
    ]
    large = [
        pltpu.make_async_copy(k_hbm.at[:, mine], keys.at[c], loc.at[5]),
        pltpu.make_async_copy(v_hbm.at[:, mine], vals.at[c], loc.at[6]),
    ]
    for copy in small + large:
        copy.start()
    mate = dev(x, y, 1 - c)

    def send_keys():
        send(k_hbm.at[:, other], keys.at[c], ex_send.at[0], ex_recv.at[0], mate)
        send(v_hbm.at[:, other], vals.at[c], ex_send.at[1], ex_recv.at[1], mate)

    barrier = pltpu.get_barrier_semaphore()

    def signal(sem, target):
        pl.semaphore_signal(
            sem, inc=1, device_id={"seq": target}, device_id_type=pl.DeviceIdType.MESH
        )

    @pl.when(rest)
    def _():
        for t in order:
            for cc in range(2):
                signal(barrier, dev(step(x, t), y, cc))
                signal(barrier, dev(x, step(y, t), cc))
        signal(barrier, dev(x, y, 1 - c))

    for copy in small:
        copy.wait()
    for h in range(H):
        rows32[h : h + 1, :] = q_in[:, h * HD : (h + 1) * HD].astype(f32)
    for g in range(KVH):
        rows32[H + g : H + g + 1, :] = kq_in[:, g * HD : (g + 1) * HD].astype(f32)
        rows32[H + KVH + g : H + KVH + g + 1, :] = vq_in[:, g * HD : (g + 1) * HD].astype(f32)
    for r in range(2):
        send_rows[r, 0] = rows32[r * HALF : (r + 1) * HALF, :].astype(bf16)
        at = H + r * KVHALF
        send_rows[r, 1] = jnp.concatenate(
            [rows32[at : at + KVHALF, :], rows32[at + KVH : at + KVH + KVHALF, :]], axis=0
        ).astype(bf16)
    got_kv[a * 2 + c] = send_rows[c, 1]

    @pl.when(rest)
    def _():
        got_q[b * 2 + c] = send_rows[c, 0]

    @pl.when(a == 0)
    def _():
        got_q[0] = jnp.zeros((HALF, HD), bf16)

    @pl.when(me == 1)
    def _():
        mate_q[0] = jnp.zeros((HALF, HD), bf16)
        mate_q[1] = send_rows[0, 0]

    line = 4 * (nb - 1) + 1
    near = jnp.where((x == 0) | (y == 0), 1, 0)
    pl.semaphore_wait(barrier, jnp.where(zero, line, line - near))

    @pl.when(zero)
    def _():
        signal(here, 1)
        for t in order:
            for cc in range(2):
                signal(here, dev(t, 0, cc))
        send_keys()
        first_q[...] = send_rows[0, 0]
        for t in order:
            for cc in range(2):
                send(send_rows.at[cc, 0], first_q, first_send, first_recv, dev(t, 0, cc))
        send(send_rows.at[1, 0], first_q, first_send, first_recv, 1)
        for t in order:
            send(send_rows.at[0, 0], first_q, first_send, first_recv, dev(0, t, 0))

    my_block = pl.ds(pl.multiple_of(a * rb, rb), rb)
    per = HALF // CHUNKS

    def send_mate_row(k, slot):
        send(send_rows.at[1 - c, k], slot, s1_send.at[k], s1_recv.at[k], mate)

    @pl.when(rest)
    def _():
        for t in order:
            to_0 = dev(x, step(y, t), 0)

            @pl.when(to_0 > 0)
            def _(to_0=to_0):
                send(send_rows.at[0, 0], got_q.at[y * 2 + c], s1_send.at[0], s1_recv.at[0], to_0)

            @pl.when(to_0 == 0)
            def _():
                send(send_rows.at[0, 0], mate_q.at[y * 2 + c], s1_send.at[0], relay_recv, 1)

            send(
                send_rows.at[1, 0], got_q.at[x * 2 + c], s1_send.at[0], s1_recv.at[0],
                dev(step(x, t), y, 1),
            )

        @pl.when(me > 1)
        def _():
            send_mate_row(0, got_q.at[a * 2 + c])

    def send_row_0(target):
        send(send_rows.at[0, 1], got_kv.at[x * 2 + c], s1_send.at[1], s1_recv.at[1], target)

    for t in order:
        to_0 = dev(step(x, t), y, 0)

        @pl.when(to_0 > 0)
        def _(to_0=to_0):
            send_row_0(to_0)

        send(
            send_rows.at[1, 1], got_kv.at[y * 2 + c], s1_send.at[1], s1_recv.at[1],
            dev(x, step(y, t), 1),
        )

    @pl.when(me != 1)
    def _():
        send_mate_row(1, got_kv.at[b * 2 + c])

    @pl.when(me > 1)
    def _():
        send_keys()

    @pl.when(rest)
    def _():
        @pl.when(a == 0)
        def _():
            await_bytes(got_q.at[0 : rb - 2], s1_recv.at[0])

        @pl.when(a > 0)
        def _():
            await_bytes(got_q.at[0 : rb - 1], s1_recv.at[0])

        for i in range(rb):
            turn32[i * HALF : (i + 1) * HALF, :] = got_q[i].astype(f32)
        for h in range(HALF):
            block = turn32[pl.ds(h, rb, stride=HALF), :].astype(bf16)
            mine_q[h] = block
            all_q[h, my_block, :] = block

        @pl.when(me == 1)
        def _():
            await_bytes(mate_q.at[2:rb], relay_recv)
            for i in range(rb):
                turn32[i * HALF : (i + 1) * HALF, :] = mate_q[i].astype(f32)
            for h in range(HALF):
                spare_q[h, 0:rb, :] = turn32[pl.ds(h, rb, stride=HALF), :].astype(bf16)
            for j in range(CHUNKS):
                some = pl.ds(j * per, per)
                for t in order:
                    send(
                        spare_q.at[some, 0:rb, :], all_q.at[some, 0:rb, :],
                        relay_send.at[0], s2_recv.at[j], dev(t, 0, 0),
                    )

        for j in range(CHUNKS):
            some = pl.ds(j * per, per)

            for t in order:
                target = role_dev(step(a, t), b, c)

                @pl.when(target > 0)
                def _(some=some, target=target, j=j):
                    send(
                        mine_q.at[some], all_q.at[some, my_block, :],
                        s2_send, s2_recv.at[j], target,
                    )

                @pl.when(target == 0)
                def _(some=some, j=j):
                    send(
                        mine_q.at[some], spare_q.at[some, my_block, :],
                        s2_send, spare_recv.at[j], 1,
                    )

    @pl.when((y == 0) & rest)
    def _():
        pl.semaphore_wait(here, 1)

        @pl.when(me == 1)
        def _():
            send_keys()
            send_mate_row(1, got_kv.at[b * 2 + c])

        @pl.when(me > 1)
        def _():
            send_row_0(0)

        await_bytes(first_q, first_recv)
        for t in order:
            send(first_q, first_q, first_send, first_recv, dev(x, t, c))

    lane = lax.broadcasted_iota(jnp.int32, (gs, 128), 1)
    for i in range(nb):
        stats[i] = jnp.full((gs, 128), NEG, f32)
    for copy in large:
        copy.wait()
    await_bytes(keys.at[1 - c], ex_recv.at[0])
    await_bytes(vals.at[1 - c], ex_recv.at[1])
    offset = off_s[0]
    places = lax.broadcasted_iota(jnp.int32, (1, doc), 1)
    seen = [places + (chip * 2 + blk) * doc < offset for blk in range(2)]
    ones = jnp.ones((doc, HD), bf16)

    def chunk(j, carry):
        first = j * per

        @pl.when(me == 1)
        def _():
            some = pl.ds(first, per)
            await_bytes(spare_q.at[some, rb:, :], spare_recv.at[j])
            send(spare_q.at[some], all_q.at[some], relay_send.at[1], s2_recv.at[j], 0)

        @pl.when(zero)
        def _():
            await_bytes(all_q.at[pl.ds(first, per)], s2_recv.at[j])

        @pl.when(rest)
        def _():
            await_bytes(all_q.at[pl.ds(first, per), 0 : (nb - 1) * rb, :], s2_recv.at[j])

        for u in range(per // GROUP):
            head = first + u * GROUP
            col = pl.ds(pl.multiple_of((head // GROUP) * HD, 128), HD)
            q = all_q[pl.ds(head, GROUP)].reshape(GROUP * rows, HD)
            tops, nums, dens = [], [], []
            for blk in range(2):
                s = lax.dot_general(
                    q, keys[blk, :, col], (((1,), (1,)), ((), ())), preferred_element_type=f32
                )
                s = jnp.where(seen[blk], s, NEG)
                top = jnp.max(s, axis=1, keepdims=True)
                p = jnp.exp2((s - top) * SCALE).astype(bf16)
                both = jnp.dot(
                    p, jnp.concatenate([vals[blk, :, col], ones], axis=1),
                    preferred_element_type=f32,
                )
                tops.append(top)
                nums.append(both[:, :HD])
                dens.append(both[:, HD:])
            top = jnp.maximum(tops[0], tops[1])
            w = [jnp.exp2((m - top) * SCALE) for m in tops]
            den = dens[0] * w[0] + dens[1] * w[1]
            inv = 1.0 / den
            o = nums[0] * (w[0] * inv) + nums[1] * (w[1] * inv)
            level = top * SCALE + jnp.log2(den)
            parts[pl.ds(head, GROUP)] = o.reshape(GROUP, rows, HD).astype(bf16)
            for i in range(nb):
                tile = stats[i]
                for z in range(GROUP):
                    for k in range(groups):
                        at = z * rows + i * rb + k * gs
                        tile = jnp.where(lane == k * HALF + head + z, level[at : at + gs], tile)
                stats[i] = tile
        for t in order:
            peer = step(a, t)
            send(
                parts.at[pl.ds(first, per), pl.ds(pl.multiple_of(peer * rb, rb), rb), :],
                got_o.at[a, pl.ds(first, per)],
                r1_send.at[0], r1_recv.at[j], role_dev(peer, b, c),
            )

            @pl.when(j == CHUNKS - 1)
            def _(peer=peer):
                send(stats.at[peer], got_l.at[a], r1_send.at[1], st_recv, role_dev(peer, b, c))

        return carry

    lax.fori_loop(0, CHUNKS, chunk, 0)
    @pl.when(y > 0)
    def _():
        await_bytes(first_q, first_recv)

    head_of = lax.broadcasted_iota(jnp.int32, (HALF, HD), 0) // GROUP
    wide = jnp.concatenate(
        [jnp.where(head_of == g, first_q[...], jnp.zeros((), bf16)) for g in range(KVHALF)], axis=1
    )
    tops, nums, dens = [], [], []
    for blk in range(2):
        s = lax.dot_general(
            wide, keys[blk], (((1,), (1,)), ((), ())), preferred_element_type=f32
        )
        s = jnp.where(seen[blk], s, NEG)
        top = jnp.max(s, axis=1, keepdims=True)
        p = jnp.exp2((s - top) * SCALE).astype(bf16)
        dens.append(jnp.sum(p.astype(f32), axis=1, keepdims=True))
        num = jnp.dot(p, vals[blk], preferred_element_type=f32)
        pick = jnp.zeros((HALF, HD), f32)
        for g in range(KVHALF):
            pick = jnp.where(head_of == g, num[:, g * HD : (g + 1) * HD], pick)
        tops.append(top)
        nums.append(pick)
    top = jnp.maximum(tops[0], tops[1])
    w = [jnp.exp2((m - top) * SCALE) for m in tops]
    den = dens[0] * w[0] + dens[1] * w[1]
    level = top * SCALE + jnp.log2(den)
    half_lane = lax.broadcasted_iota(jnp.int32, (HALF // 2, 128), 1) < 64

    def paired(v):
        return jnp.where(half_lane, v[: HALF // 2], v[HALF // 2 :])

    first_o[a] = ((nums[0] * w[0] + nums[1] * w[1]) / den).astype(bf16)
    first_l[a] = paired(level)

    @pl.when(a > 0)
    def _():
        target = role_dev(0, b, c)
        send(first_o.at[a], first_o.at[a], back_send.at[0], back_recv.at[0], target)
        send(first_l.at[a], first_l.at[a], back_send.at[1], back_recv.at[1], target)

    await_bytes(got_kv.at[0 : rb - 1], s1_recv.at[1])
    for i in range(rb):
        turn32[i * HALF : (i + 1) * HALF, :] = got_kv[i].astype(f32)

    def row_of(aa, bb, cc):
        return dev(aa * (1 - c) + bb * c, bb * (1 - c) + aa * c, cc)

    spot = lax.rem(lax.broadcasted_iota(jnp.int32, (GROUP * rb, rb), 0), rb)
    key_spot = lax.broadcasted_iota(jnp.int32, (GROUP * rb, rb), 1)
    see = row_of(key_spot // 2, b, lax.rem(key_spot, 2)) <= row_of(a, spot // 2, lax.rem(spot, 2))
    own = jnp.full((gs, 128), NEG, f32)
    for g in range(KVHALF):
        key = turn32[pl.ds(g, rb, stride=HALF), :].astype(bf16)
        val = turn32[pl.ds(KVHALF + g, rb, stride=HALF), :].astype(bf16)
        q = all_q[g * GROUP : (g + 1) * GROUP, my_block, :].reshape(GROUP * rb, HD)
        s = lax.dot_general(q, key, (((1,), (1,)), ((), ())), preferred_element_type=f32)
        s = jnp.where(see, s, NEG)
        top = jnp.max(s, axis=1, keepdims=True)
        p = jnp.exp2((s - top) * SCALE).astype(bf16)
        den = jnp.sum(p.astype(f32), axis=1, keepdims=True)
        num = jnp.dot(p, val, preferred_element_type=f32)
        own_o[g * GROUP : (g + 1) * GROUP] = (num / den).reshape(GROUP, rb, HD)
        level = top * SCALE + jnp.log2(den)
        for i in range(GROUP):
            for k in range(groups):
                at = i * rb + k * gs
                own = jnp.where(lane == k * HALF + g * GROUP + i, level[at : at + gs], own)
    own_l[...] = own

    await_bytes(got_l.at[0 : nb - 1], st_recv)
    levels = [stats[a]] + [got_l[step(a, t)] for t in range(1, nb)] + [own_l[...]]
    top = functools.reduce(jnp.maximum, levels)
    weights = [jnp.exp2(v - top) for v in levels]
    total = functools.reduce(jnp.add, weights)
    inv = 1.0 / total
    weights = [w * inv for w in weights]
    level = top + jnp.log2(total)
    for j in range(CHUNKS):
        await_bytes(got_o.at[0 : nb - 1, pl.ds(j * per, per)], r1_recv.at[j])
        for h in range(j * per, (j + 1) * per):
            full = [parts[h, pl.ds(pl.multiple_of(a * rb, rb), rb), :].astype(f32)]
            full += [got_o[step(a, t), h].astype(f32) for t in range(1, nb)]
            full += [own_o[h]]
            for k in range(groups):
                at = k * HALF + h
                acc = weights[0][:, at : at + 1] * full[0][k * gs : (k + 1) * gs]
                for w, part in zip(weights[1:], full[1:]):
                    acc += w[:, at : at + 1] * part[k * gs : (k + 1) * gs]
                row_o[pl.ds(k * gs * ROW_TILES + h, gs, stride=ROW_TILES), :] = acc
    for h in range(HALF // 2):
        for k in range(groups):
            at = k * HALF + h
            pair = jnp.where(
                lane < 64, level[:, at : at + 1], level[:, at + HALF // 2 : at + HALF // 2 + 1]
            )
            row_o[pl.ds(k * gs * ROW_TILES + HALF + h, gs, stride=ROW_TILES), :] = pair

    def row_at(i):
        return pl.ds(pl.multiple_of(i * ROW_TILES, 8), ROW_TILES)

    def spread(w, k):
        return w[:, k * 64 : k * 64 + 1]

    def merged(levels, values):
        top = functools.reduce(jnp.maximum, levels)
        weights = [jnp.exp2(v - top) for v in levels]
        total = functools.reduce(jnp.add, weights)
        inv = 1.0 / total
        outs = []
        for k in range(2):
            terms = [
                spread(w * inv, k) * v[k * HALF // 2 : (k + 1) * HALF // 2]
                for w, v in zip(weights, values)
            ]
            outs.append(functools.reduce(jnp.add, terms))
        return jnp.concatenate(outs, axis=0), top + jnp.log2(total)

    mine_last = last.at[c * nb + b]
    for t in order:
        peer = step(b, t)
        for cc in range(2):
            target = role_dev(a, peer, cc)

            @pl.when(target > 0)
            def _(row=peer * 2 + cc, target=target):
                send(row_o.at[row_at(row)], mine_last, r2_send, r2_recv, target)

    @pl.when(me != 1)
    def _():
        send(row_o.at[row_at(b * 2 + 1 - c)], mine_last, r2_send, r2_recv, mate)

    mine_last[...] = row_o[row_at(b * 2 + c), :]

    @pl.when(a == 0)
    def _():
        await_bytes(first_o.at[0 : nb - 1], back_recv.at[0])
        await_bytes(first_l.at[0 : nb - 1], back_recv.at[1])
        pair = got_kv[0].astype(f32)
        for i in range(GROUP):
            pair_k[pl.ds(i, KVHALF, stride=GROUP), :] = pair[:KVHALF]
            pair_v[pl.ds(i, KVHALF, stride=GROUP), :] = pair[KVHALF:]
        score = jnp.sum(first_q[...].astype(f32) * pair_k[...], axis=1, keepdims=True) * SCALE
        score = jnp.where(jnp.full((HALF // 2, 128), b, jnp.int32) == 0, paired(score), NEG)
        values, level = merged(
            [first_l[i] for i in range(nb)] + [score],
            [first_o[i].astype(f32) for i in range(nb)] + [pair_v[...]],
        )
        row_o[0:HALF, :] = values
        row_o[HALF:ROW_TILES, :] = level

        @pl.when(zero)
        def _():
            mine_last[...] = row_o[0:ROW_TILES, :]

        @pl.when(rest)
        def _():
            send(row_o.at[0:ROW_TILES], mine_last, r2_send, r2_recv, 0)

    await_bytes(last.at[0 : 2 * nb - 1], r2_recv)

    live = jnp.full((HALF, 128), me, jnp.int32) < len_s[0]
    for r in range(2):
        got = [last[r * nb + i] for i in range(nb)]
        values, _ = merged([v[HALF:] for v in got], [v[:HALF] for v in got])
        out_ref[r * HALF : (r + 1) * HALF, :] = jnp.where(live, values, 0.0).astype(bf16)

    @pl.when(me == 1)
    def _():
        await_bytes(got_q.at[0 : rb - 2], s1_send.at[0])

    @pl.when(me > 1)
    def _():
        await_bytes(got_q.at[0 : rb - 1], s1_send.at[0])

    await_bytes(got_kv.at[0 : rb - 1], s1_send.at[1])
    for i, buf in enumerate((keys, vals)):
        await_bytes(buf.at[c], ex_send.at[i])
    await_bytes(got_o.at[0 : nb - 1], r1_send.at[0])
    await_bytes(got_l.at[0 : nb - 1], r1_send.at[1])

    @pl.when(rest)
    def _():
        await_bytes(all_q.at[:, 0 : (nb - 1) * rb, :], s2_send)

    @pl.when(a > 0)
    def _():
        await_bytes(first_o.at[a], back_send.at[0])
        await_bytes(first_l.at[a], back_send.at[1])

    @pl.when(me == 1)
    def _():
        await_bytes(all_q.at[:, rb:, :], relay_send.at[0])
        await_bytes(all_q, relay_send.at[1])

    await_bytes(last.at[0 : 2 * nb - 1], r2_send)

    @pl.when(zero)
    def _():
        await_bytes(got_q.at[0 : rb - 1], first_send)

    @pl.when(y == 0)
    def _():
        await_bytes(got_q.at[0 : nb - 1], first_send)


def local(nb, q, kq, vq, k, v, lengths, offsets):
    rb = 2 * nb
    rows = rb * nb
    doc = k.shape[0]
    gs = rb // max(rb // 8, 1)
    dma = pltpu.SemaphoreType.DMA
    out = pl.pallas_call(
        functools.partial(kernel, nb),
        out_shape=pltpu.VMEM((H, HD), bf16),
        in_specs=[pl.BlockSpec(memory_space=pltpu.HBM)] * 7,
        out_specs=pl.BlockSpec(memory_space=pltpu.VMEM),
        scratch_shapes=[
            pltpu.VMEM((1, H * HD), bf16),
            pltpu.VMEM((1, KVH * HD), bf16),
            pltpu.VMEM((1, KVH * HD), bf16),
            pltpu.SMEM((1,), jnp.int32),
            pltpu.SMEM((1,), jnp.int32),
            pltpu.VMEM((H + 2 * KVH, HD), f32),
            pltpu.VMEM((2, 2, HALF, HD), bf16),
            pltpu.VMEM((rb, HALF, HD), bf16),
            pltpu.VMEM((rb, HALF, HD), bf16),
            pltpu.VMEM((rb * HALF, HD), f32),
            pltpu.VMEM((HALF, rb, HD), bf16),
            pltpu.VMEM((HALF, rows, HD), bf16),
            pltpu.VMEM((2, doc, KVHALF * HD), bf16),
            pltpu.VMEM((2, doc, KVHALF * HD), bf16),
            pltpu.VMEM((HALF, rows, HD), bf16),
            pltpu.VMEM((nb, gs, 128), f32),
            pltpu.VMEM((HALF, rb, HD), f32),
            pltpu.VMEM((gs, 128), f32),
            pltpu.VMEM((nb, HALF, rb, HD), bf16),
            pltpu.VMEM((nb, gs, 128), f32),
            pltpu.VMEM((rb * ROW_TILES, HD), f32),
            pltpu.VMEM((2 * nb, ROW_TILES, HD), f32),
            pltpu.VMEM((rb, HALF, HD), bf16),
            pltpu.VMEM((HALF, rows, HD), bf16),
            pltpu.VMEM((HALF, HD), bf16),
            pltpu.VMEM((nb, HALF, HD), bf16),
            pltpu.VMEM((nb, HALF // 2, HD), f32),
            pltpu.VMEM((HALF, HD), f32),
            pltpu.VMEM((HALF, HD), f32),
            dma((7,)), dma((2,)), dma((2,)), dma((2,)), dma((2,)), dma, dma((CHUNKS,)),
            dma((2,)), dma((CHUNKS,)), dma, dma, dma,
            pltpu.SemaphoreType.REGULAR, dma((CHUNKS,)), dma, dma((2,)), dma, dma, dma((2,)), dma((2,)),
        ],
        compiler_params=pltpu.CompilerParams(
            collective_id=0, has_side_effects=True, vmem_limit_bytes=56 * 1024 * 1024
        ),
    )(q, kq, vq, k, v, lengths, offsets)
    return out.reshape(1, H * HD)


def solution(mesh):
    nb = math.isqrt(mesh.shape["seq"] // 2)
    rows = P(("grp", "seq"), None)
    return jax.shard_map(
        functools.partial(local, nb),
        mesh=mesh,
        in_specs=(rows, rows, rows, rows, rows, P("grp"), P("grp")),
        out_specs=rows,
        check_vma=False,
    )
```

```python
import functools
import math

import jax
import jax.numpy as jnp
from jax import lax
from jax.experimental import pallas as pl
from jax.experimental.pallas import tpu as pltpu
from jax.sharding import PartitionSpec as P

H = 32
KVH = 16
HD = 128
QSCALE = 144
NEG = -1e30
HALF = H // 2
KVHALF = KVH // 2
GROUP = H // KVH
SCALE = QSCALE ** (-0.5) * math.log2(math.e)
CHUNKS = 4
ROW_TILES = 24

f32 = jnp.float32
bf16 = jnp.bfloat16


def kernel(
    nb,
    q_hbm, kq_hbm, vq_hbm, k_hbm, v_hbm, len_hbm, off_hbm,
    out_ref,
    q_in, kq_in, vq_in, len_s, off_s, rows32, send_rows, got_q, got_kv, turn32,
    mine_q, all_q, keys, vals, parts, stats, own_o, own_l, got_o, got_l, row_o, last,
    mate_q, spare_q, first_q, first_o, first_l, pair_k, pair_v,
    loc, ex_send, ex_recv, s1_send, s1_recv, s2_send, s2_recv,
    r1_send, r1_recv, st_recv, r2_send, r2_recv,
    here, spare_recv, relay_recv, relay_send, first_send, first_recv, back_send, back_recv,
):
    rb = 2 * nb
    rows = rb * nb
    groups = max(rb // 8, 1)
    gs = rb // groups
    doc = k_hbm.shape[0]
    width = KVHALF * HD
    me = lax.axis_index("seq")
    c = lax.rem(me, 2)
    chip = me // 2
    x = lax.rem(chip, nb)
    y = chip // nb
    a = x * (1 - c) + y * c
    b = y * (1 - c) + x * c

    def dev(xx, yy, cc):
        return (yy * nb + xx) * 2 + cc

    def role_dev(aa, bb, cc):
        return dev(aa * (1 - c) + bb * c, bb * (1 - c) + aa * c, cc)

    def step(v, t):
        return lax.rem(v + t, nb)

    zero = me == 0
    rest = me > 0
    order = sorted(range(1, nb), key=lambda t: -min(t, nb - t))

    def send(src, dst, ssem, rsem, target):
        pltpu.make_async_remote_copy(
            src_ref=src, dst_ref=dst, send_sem=ssem, recv_sem=rsem,
            device_id={"seq": target}, device_id_type=pl.DeviceIdType.MESH,
        ).start()

    def await_bytes(ref, sem):
        pltpu.make_async_copy(ref, ref, sem).wait()

    mine = pl.ds(pl.multiple_of(c * width, 128), width)
    other = pl.ds(pl.multiple_of((1 - c) * width, 128), width)
    small = [
        pltpu.make_async_copy(q_hbm, q_in, loc.at[0]),
        pltpu.make_async_copy(kq_hbm, kq_in, loc.at[1]),
        pltpu.make_async_copy(vq_hbm, vq_in, loc.at[2]),
        pltpu.make_async_copy(len_hbm, len_s, loc.at[3]),
        pltpu.make_async_copy(off_hbm, off_s, loc.at[4]),
    ]
    large = [
        pltpu.make_async_copy(k_hbm.at[:, mine], keys.at[c], loc.at[5]),
        pltpu.make_async_copy(v_hbm.at[:, mine], vals.at[c], loc.at[6]),
    ]
    for copy in small:
        copy.start()
    mate = dev(x, y, 1 - c)

    def send_keys():
        send(k_hbm.at[:, other], keys.at[c], ex_send.at[0], ex_recv.at[0], mate)
        send(v_hbm.at[:, other], vals.at[c], ex_send.at[1], ex_recv.at[1], mate)

    barrier = pltpu.get_barrier_semaphore()

    def signal(sem, target):
        pl.semaphore_signal(
            sem, inc=1, device_id={"seq": target}, device_id_type=pl.DeviceIdType.MESH
        )

    @pl.when(rest)
    def _():
        for t in order:
            for cc in range(2):
                signal(barrier, dev(step(x, t), y, cc))
                signal(barrier, dev(x, step(y, t), cc))
        signal(barrier, dev(x, y, 1 - c))

    for copy in large:
        copy.start()
    for copy in small:
        copy.wait()
    for h in range(H):
        rows32[h : h + 1, :] = q_in[:, h * HD : (h + 1) * HD].astype(f32)
    for g in range(KVH):
        rows32[H + g : H + g + 1, :] = kq_in[:, g * HD : (g + 1) * HD].astype(f32)
        rows32[H + KVH + g : H + KVH + g + 1, :] = vq_in[:, g * HD : (g + 1) * HD].astype(f32)
    for r in range(2):
        send_rows[r, 0] = rows32[r * HALF : (r + 1) * HALF, :].astype(bf16)
        at = H + r * KVHALF
        send_rows[r, 1] = jnp.concatenate(
            [rows32[at : at + KVHALF, :], rows32[at + KVH : at + KVH + KVHALF, :]], axis=0
        ).astype(bf16)
    got_kv[a * 2 + c] = send_rows[c, 1]

    @pl.when(rest)
    def _():
        got_q[b * 2 + c] = send_rows[c, 0]

    @pl.when(a == 0)
    def _():
        got_q[0] = jnp.zeros((HALF, HD), bf16)

    @pl.when(me == 1)
    def _():
        mate_q[0] = jnp.zeros((HALF, HD), bf16)
        mate_q[1] = send_rows[0, 0]

    line = 4 * (nb - 1) + 1
    near = jnp.where((x == 0) | (y == 0), 1, 0)
    pl.semaphore_wait(barrier, jnp.where(zero, line, line - near))

    @pl.when(zero)
    def _():
        signal(here, 1)
        for t in order:
            for cc in range(2):
                signal(here, dev(t, 0, cc))
        send_keys()
        first_q[...] = send_rows[0, 0]
        for t in order:
            for cc in range(2):
                send(send_rows.at[cc, 0], first_q, first_send, first_recv, dev(t, 0, cc))
        send(send_rows.at[1, 0], first_q, first_send, first_recv, 1)
        for t in order:
            send(send_rows.at[0, 0], first_q, first_send, first_recv, dev(0, t, 0))

    my_block = pl.ds(pl.multiple_of(a * rb, rb), rb)
    per = HALF // CHUNKS

    def send_mate_row(k, slot):
        send(send_rows.at[1 - c, k], slot, s1_send.at[k], s1_recv.at[k], mate)

    @pl.when(rest)
    def _():
        for t in order:
            to_0 = dev(x, step(y, t), 0)

            @pl.when(to_0 > 0)
            def _(to_0=to_0):
                send(send_rows.at[0, 0], got_q.at[y * 2 + c], s1_send.at[0], s1_recv.at[0], to_0)

            @pl.when(to_0 == 0)
            def _():
                send(send_rows.at[0, 0], mate_q.at[y * 2 + c], s1_send.at[0], relay_recv, 1)

            send(
                send_rows.at[1, 0], got_q.at[x * 2 + c], s1_send.at[0], s1_recv.at[0],
                dev(step(x, t), y, 1),
            )

        @pl.when(me > 1)
        def _():
            send_mate_row(0, got_q.at[a * 2 + c])

    def send_row_0(target):
        send(send_rows.at[0, 1], got_kv.at[x * 2 + c], s1_send.at[1], s1_recv.at[1], target)

    for t in order:
        to_0 = dev(step(x, t), y, 0)

        @pl.when(to_0 > 0)
        def _(to_0=to_0):
            send_row_0(to_0)

        send(
            send_rows.at[1, 1], got_kv.at[y * 2 + c], s1_send.at[1], s1_recv.at[1],
            dev(x, step(y, t), 1),
        )

    @pl.when(me != 1)
    def _():
        send_mate_row(1, got_kv.at[b * 2 + c])

    @pl.when(me > 1)
    def _():
        send_keys()

    @pl.when(rest)
    def _():
        @pl.when(a == 0)
        def _():
            await_bytes(got_q.at[0 : rb - 2], s1_recv.at[0])

        @pl.when(a > 0)
        def _():
            await_bytes(got_q.at[0 : rb - 1], s1_recv.at[0])

        for i in range(rb):
            turn32[i * HALF : (i + 1) * HALF, :] = got_q[i].astype(f32)
        for h in range(HALF):
            block = turn32[pl.ds(h, rb, stride=HALF), :].astype(bf16)
            mine_q[h] = block
            all_q[h, my_block, :] = block

        @pl.when(me == 1)
        def _():
            await_bytes(mate_q.at[2:rb], relay_recv)
            for i in range(rb):
                turn32[i * HALF : (i + 1) * HALF, :] = mate_q[i].astype(f32)
            for h in range(HALF):
                spare_q[h, 0:rb, :] = turn32[pl.ds(h, rb, stride=HALF), :].astype(bf16)
            for j in range(CHUNKS):
                some = pl.ds(j * per, per)
                for t in order:
                    send(
                        spare_q.at[some, 0:rb, :], all_q.at[some, 0:rb, :],
                        relay_send.at[0], s2_recv.at[j], dev(t, 0, 0),
                    )

        for j in range(CHUNKS):
            some = pl.ds(j * per, per)

            for t in order:
                target = role_dev(step(a, t), b, c)

                @pl.when(target > 0)
                def _(some=some, target=target, j=j):
                    send(
                        mine_q.at[some], all_q.at[some, my_block, :],
                        s2_send, s2_recv.at[j], target,
                    )

                @pl.when(target == 0)
                def _(some=some, j=j):
                    send(
                        mine_q.at[some], spare_q.at[some, my_block, :],
                        s2_send, spare_recv.at[j], 1,
                    )

    @pl.when((y == 0) & rest)
    def _():
        pl.semaphore_wait(here, 1)

        @pl.when(me == 1)
        def _():
            send_keys()
            send_mate_row(1, got_kv.at[b * 2 + c])

        @pl.when(me > 1)
        def _():
            send_row_0(0)

        await_bytes(first_q, first_recv)
        for t in order:
            send(first_q, first_q, first_send, first_recv, dev(x, t, c))

    lane = lax.broadcasted_iota(jnp.int32, (gs, 128), 1)
    for i in range(nb):
        stats[i] = jnp.full((gs, 128), NEG, f32)
    for copy in large:
        copy.wait()
    await_bytes(keys.at[1 - c], ex_recv.at[0])
    await_bytes(vals.at[1 - c], ex_recv.at[1])
    offset = off_s[0]
    places = lax.broadcasted_iota(jnp.int32, (1, doc), 1)
    seen = [places + (chip * 2 + blk) * doc < offset for blk in range(2)]
    ones = jnp.ones((doc, HD), bf16)

    def chunk(j, carry):
        first = j * per

        @pl.when(me == 1)
        def _():
            some = pl.ds(first, per)
            await_bytes(spare_q.at[some, rb:, :], spare_recv.at[j])
            send(spare_q.at[some], all_q.at[some], relay_send.at[1], s2_recv.at[j], 0)

        @pl.when(zero)
        def _():
            await_bytes(all_q.at[pl.ds(first, per)], s2_recv.at[j])

        @pl.when(rest)
        def _():
            await_bytes(all_q.at[pl.ds(first, per), 0 : (nb - 1) * rb, :], s2_recv.at[j])

        for u in range(per // GROUP):
            head = first + u * GROUP
            col = pl.ds(pl.multiple_of((head // GROUP) * HD, 128), HD)
            q = all_q[pl.ds(head, GROUP)].reshape(GROUP * rows, HD)
            tops, nums, dens = [], [], []
            for blk in range(2):
                s = lax.dot_general(
                    q, keys[blk, :, col], (((1,), (1,)), ((), ())), preferred_element_type=f32
                )
                s = jnp.where(seen[blk], s, NEG)
                top = jnp.max(s, axis=1, keepdims=True)
                p = jnp.exp2((s - top) * SCALE).astype(bf16)
                both = jnp.dot(
                    p, jnp.concatenate([vals[blk, :, col], ones], axis=1),
                    preferred_element_type=f32,
                )
                tops.append(top)
                nums.append(both[:, :HD])
                dens.append(both[:, HD:])
            top = jnp.maximum(tops[0], tops[1])
            w = [jnp.exp2((m - top) * SCALE) for m in tops]
            den = dens[0] * w[0] + dens[1] * w[1]
            inv = 1.0 / den
            o = nums[0] * (w[0] * inv) + nums[1] * (w[1] * inv)
            level = top * SCALE + jnp.log2(den)
            parts[pl.ds(head, GROUP)] = o.reshape(GROUP, rows, HD).astype(bf16)
            for i in range(nb):
                tile = stats[i]
                for z in range(GROUP):
                    for k in range(groups):
                        at = z * rows + i * rb + k * gs
                        tile = jnp.where(lane == k * HALF + head + z, level[at : at + gs], tile)
                stats[i] = tile
        for t in order:
            peer = step(a, t)
            send(
                parts.at[pl.ds(first, per), pl.ds(pl.multiple_of(peer * rb, rb), rb), :],
                got_o.at[a, pl.ds(first, per)],
                r1_send.at[0], r1_recv.at[j], role_dev(peer, b, c),
            )

            @pl.when(j == CHUNKS - 1)
            def _(peer=peer):
                send(stats.at[peer], got_l.at[a], r1_send.at[1], st_recv, role_dev(peer, b, c))

        return carry

    lax.fori_loop(0, CHUNKS, chunk, 0)
    @pl.when(y > 0)
    def _():
        await_bytes(first_q, first_recv)

    head_of = lax.broadcasted_iota(jnp.int32, (HALF, HD), 0) // GROUP
    wide = jnp.concatenate(
        [jnp.where(head_of == g, first_q[...], jnp.zeros((), bf16)) for g in range(KVHALF)], axis=1
    )
    tops, nums, dens = [], [], []
    for blk in range(2):
        s = lax.dot_general(
            wide, keys[blk], (((1,), (1,)), ((), ())), preferred_element_type=f32
        )
        s = jnp.where(seen[blk], s, NEG)
        top = jnp.max(s, axis=1, keepdims=True)
        p = jnp.exp2((s - top) * SCALE).astype(bf16)
        dens.append(jnp.sum(p.astype(f32), axis=1, keepdims=True))
        num = jnp.dot(p, vals[blk], preferred_element_type=f32)
        pick = jnp.zeros((HALF, HD), f32)
        for g in range(KVHALF):
            pick = jnp.where(head_of == g, num[:, g * HD : (g + 1) * HD], pick)
        tops.append(top)
        nums.append(pick)
    top = jnp.maximum(tops[0], tops[1])
    w = [jnp.exp2((m - top) * SCALE) for m in tops]
    den = dens[0] * w[0] + dens[1] * w[1]
    level = top * SCALE + jnp.log2(den)
    half_lane = lax.broadcasted_iota(jnp.int32, (HALF // 2, 128), 1) < 64

    def paired(v):
        return jnp.where(half_lane, v[: HALF // 2], v[HALF // 2 :])

    first_o[a] = ((nums[0] * w[0] + nums[1] * w[1]) / den).astype(bf16)
    first_l[a] = paired(level)

    @pl.when(a > 0)
    def _():
        target = role_dev(0, b, c)
        send(first_o.at[a], first_o.at[a], back_send.at[0], back_recv.at[0], target)
        send(first_l.at[a], first_l.at[a], back_send.at[1], back_recv.at[1], target)

    await_bytes(got_kv.at[0 : rb - 1], s1_recv.at[1])
    for i in range(rb):
        turn32[i * HALF : (i + 1) * HALF, :] = got_kv[i].astype(f32)

    def row_of(aa, bb, cc):
        return dev(aa * (1 - c) + bb * c, bb * (1 - c) + aa * c, cc)

    spot = lax.rem(lax.broadcasted_iota(jnp.int32, (GROUP * rb, rb), 0), rb)
    key_spot = lax.broadcasted_iota(jnp.int32, (GROUP * rb, rb), 1)
    see = row_of(key_spot // 2, b, lax.rem(key_spot, 2)) <= row_of(a, spot // 2, lax.rem(spot, 2))
    own = jnp.full((gs, 128), NEG, f32)
    for g in range(KVHALF):
        key = turn32[pl.ds(g, rb, stride=HALF), :].astype(bf16)
        val = turn32[pl.ds(KVHALF + g, rb, stride=HALF), :].astype(bf16)
        q = all_q[g * GROUP : (g + 1) * GROUP, my_block, :].reshape(GROUP * rb, HD)
        s = lax.dot_general(q, key, (((1,), (1,)), ((), ())), preferred_element_type=f32)
        s = jnp.where(see, s, NEG)
        top = jnp.max(s, axis=1, keepdims=True)
        p = jnp.exp2((s - top) * SCALE).astype(bf16)
        den = jnp.sum(p.astype(f32), axis=1, keepdims=True)
        num = jnp.dot(p, val, preferred_element_type=f32)
        own_o[g * GROUP : (g + 1) * GROUP] = (num / den).reshape(GROUP, rb, HD)
        level = top * SCALE + jnp.log2(den)
        for i in range(GROUP):
            for k in range(groups):
                at = i * rb + k * gs
                own = jnp.where(lane == k * HALF + g * GROUP + i, level[at : at + gs], own)
    own_l[...] = own

    await_bytes(got_l.at[0 : nb - 1], st_recv)
    levels = [stats[a]] + [got_l[step(a, t)] for t in range(1, nb)] + [own_l[...]]
    top = functools.reduce(jnp.maximum, levels)
    weights = [jnp.exp2(v - top) for v in levels]
    total = functools.reduce(jnp.add, weights)
    inv = 1.0 / total
    weights = [w * inv for w in weights]
    level = top + jnp.log2(total)
    for j in range(CHUNKS):
        await_bytes(got_o.at[0 : nb - 1, pl.ds(j * per, per)], r1_recv.at[j])
        for h in range(j * per, (j + 1) * per):
            full = [parts[h, pl.ds(pl.multiple_of(a * rb, rb), rb), :].astype(f32)]
            full += [got_o[step(a, t), h].astype(f32) for t in range(1, nb)]
            full += [own_o[h]]
            for k in range(groups):
                at = k * HALF + h
                acc = weights[0][:, at : at + 1] * full[0][k * gs : (k + 1) * gs]
                for w, part in zip(weights[1:], full[1:]):
                    acc += w[:, at : at + 1] * part[k * gs : (k + 1) * gs]
                row_o[pl.ds(k * gs * ROW_TILES + h, gs, stride=ROW_TILES), :] = acc
    for h in range(HALF // 2):
        for k in range(groups):
            at = k * HALF + h
            pair = jnp.where(
                lane < 64, level[:, at : at + 1], level[:, at + HALF // 2 : at + HALF // 2 + 1]
            )
            row_o[pl.ds(k * gs * ROW_TILES + HALF + h, gs, stride=ROW_TILES), :] = pair

    def row_at(i):
        return pl.ds(pl.multiple_of(i * ROW_TILES, 8), ROW_TILES)

    def spread(w, k):
        return w[:, k * 64 : k * 64 + 1]

    def merged(levels, values):
        top = functools.reduce(jnp.maximum, levels)
        weights = [jnp.exp2(v - top) for v in levels]
        total = functools.reduce(jnp.add, weights)
        inv = 1.0 / total
        outs = []
        for k in range(2):
            terms = [
                spread(w * inv, k) * v[k * HALF // 2 : (k + 1) * HALF // 2]
                for w, v in zip(weights, values)
            ]
            outs.append(functools.reduce(jnp.add, terms))
        return jnp.concatenate(outs, axis=0), top + jnp.log2(total)

    mine_last = last.at[c * nb + b]
    for t in order:
        peer = step(b, t)
        for cc in range(2):
            target = role_dev(a, peer, cc)

            @pl.when(target > 0)
            def _(row=peer * 2 + cc, target=target):
                send(row_o.at[row_at(row)], mine_last, r2_send, r2_recv, target)

    @pl.when(me != 1)
    def _():
        send(row_o.at[row_at(b * 2 + 1 - c)], mine_last, r2_send, r2_recv, mate)

    mine_last[...] = row_o[row_at(b * 2 + c), :]

    @pl.when(a == 0)
    def _():
        await_bytes(first_o.at[0 : nb - 1], back_recv.at[0])
        await_bytes(first_l.at[0 : nb - 1], back_recv.at[1])
        pair = got_kv[0].astype(f32)
        for i in range(GROUP):
            pair_k[pl.ds(i, KVHALF, stride=GROUP), :] = pair[:KVHALF]
            pair_v[pl.ds(i, KVHALF, stride=GROUP), :] = pair[KVHALF:]
        score = jnp.sum(first_q[...].astype(f32) * pair_k[...], axis=1, keepdims=True) * SCALE
        score = jnp.where(jnp.full((HALF // 2, 128), b, jnp.int32) == 0, paired(score), NEG)
        values, level = merged(
            [first_l[i] for i in range(nb)] + [score],
            [first_o[i].astype(f32) for i in range(nb)] + [pair_v[...]],
        )
        row_o[0:HALF, :] = values
        row_o[HALF:ROW_TILES, :] = level

        @pl.when(zero)
        def _():
            mine_last[...] = row_o[0:ROW_TILES, :]

        @pl.when(rest)
        def _():
            send(row_o.at[0:ROW_TILES], mine_last, r2_send, r2_recv, 0)

    await_bytes(last.at[0 : 2 * nb - 1], r2_recv)

    live = jnp.full((HALF, 128), me, jnp.int32) < len_s[0]
    for r in range(2):
        got = [last[r * nb + i] for i in range(nb)]
        values, _ = merged([v[HALF:] for v in got], [v[:HALF] for v in got])
        out_ref[r * HALF : (r + 1) * HALF, :] = jnp.where(live, values, 0.0).astype(bf16)

    @pl.when(me == 1)
    def _():
        await_bytes(got_q.at[0 : rb - 2], s1_send.at[0])

    @pl.when(me > 1)
    def _():
        await_bytes(got_q.at[0 : rb - 1], s1_send.at[0])

    await_bytes(got_kv.at[0 : rb - 1], s1_send.at[1])
    for i, buf in enumerate((keys, vals)):
        await_bytes(buf.at[c], ex_send.at[i])
    await_bytes(got_o.at[0 : nb - 1], r1_send.at[0])
    await_bytes(got_l.at[0 : nb - 1], r1_send.at[1])

    @pl.when(rest)
    def _():
        await_bytes(all_q.at[:, 0 : (nb - 1) * rb, :], s2_send)

    @pl.when(a > 0)
    def _():
        await_bytes(first_o.at[a], back_send.at[0])
        await_bytes(first_l.at[a], back_send.at[1])

    @pl.when(me == 1)
    def _():
        await_bytes(all_q.at[:, rb:, :], relay_send.at[0])
        await_bytes(all_q, relay_send.at[1])

    await_bytes(last.at[0 : 2 * nb - 1], r2_send)

    @pl.when(zero)
    def _():
        await_bytes(got_q.at[0 : rb - 1], first_send)

    @pl.when(y == 0)
    def _():
        await_bytes(got_q.at[0 : nb - 1], first_send)


def local(nb, q, kq, vq, k, v, lengths, offsets):
    rb = 2 * nb
    rows = rb * nb
    doc = k.shape[0]
    gs = rb // max(rb // 8, 1)
    dma = pltpu.SemaphoreType.DMA
    out = pl.pallas_call(
        functools.partial(kernel, nb),
        out_shape=pltpu.VMEM((H, HD), bf16),
        in_specs=[pl.BlockSpec(memory_space=pltpu.HBM)] * 7,
        out_specs=pl.BlockSpec(memory_space=pltpu.VMEM),
        scratch_shapes=[
            pltpu.VMEM((1, H * HD), bf16),
            pltpu.VMEM((1, KVH * HD), bf16),
            pltpu.VMEM((1, KVH * HD), bf16),
            pltpu.SMEM((1,), jnp.int32),
            pltpu.SMEM((1,), jnp.int32),
            pltpu.VMEM((H + 2 * KVH, HD), f32),
            pltpu.VMEM((2, 2, HALF, HD), bf16),
            pltpu.VMEM((rb, HALF, HD), bf16),
            pltpu.VMEM((rb, HALF, HD), bf16),
            pltpu.VMEM((rb * HALF, HD), f32),
            pltpu.VMEM((HALF, rb, HD), bf16),
            pltpu.VMEM((HALF, rows, HD), bf16),
            pltpu.VMEM((2, doc, KVHALF * HD), bf16),
            pltpu.VMEM((2, doc, KVHALF * HD), bf16),
            pltpu.VMEM((HALF, rows, HD), bf16),
            pltpu.VMEM((nb, gs, 128), f32),
            pltpu.VMEM((HALF, rb, HD), f32),
            pltpu.VMEM((gs, 128), f32),
            pltpu.VMEM((nb, HALF, rb, HD), bf16),
            pltpu.VMEM((nb, gs, 128), f32),
            pltpu.VMEM((rb * ROW_TILES, HD), f32),
            pltpu.VMEM((2 * nb, ROW_TILES, HD), f32),
            pltpu.VMEM((rb, HALF, HD), bf16),
            pltpu.VMEM((HALF, rows, HD), bf16),
            pltpu.VMEM((HALF, HD), bf16),
            pltpu.VMEM((nb, HALF, HD), bf16),
            pltpu.VMEM((nb, HALF // 2, HD), f32),
            pltpu.VMEM((HALF, HD), f32),
            pltpu.VMEM((HALF, HD), f32),
            dma((7,)), dma((2,)), dma((2,)), dma((2,)), dma((2,)), dma, dma((CHUNKS,)),
            dma((2,)), dma((CHUNKS,)), dma, dma, dma,
            pltpu.SemaphoreType.REGULAR, dma((CHUNKS,)), dma, dma((2,)), dma, dma, dma((2,)), dma((2,)),
        ],
        compiler_params=pltpu.CompilerParams(
            collective_id=0, has_side_effects=True, vmem_limit_bytes=56 * 1024 * 1024
        ),
    )(q, kq, vq, k, v, lengths, offsets)
    return out.reshape(1, H * HD)


def solution(mesh):
    nb = math.isqrt(mesh.shape["seq"] // 2)
    rows = P(("grp", "seq"), None)
    return jax.shard_map(
        functools.partial(local, nb),
        mesh=mesh,
        in_specs=(rows, rows, rows, rows, rows, P("grp"), P("grp")),
        out_specs=rows,
        check_vma=False,
    )
```

```python
import functools
import math

import jax
import jax.numpy as jnp
from jax import lax
from jax.experimental import pallas as pl
from jax.experimental.pallas import tpu as pltpu
from jax.sharding import PartitionSpec as P

H = 32
KVH = 16
HD = 128
QSCALE = 144
NEG = -1e30
HALF = H // 2
KVHALF = KVH // 2
GROUP = H // KVH
SCALE = QSCALE ** (-0.5) * math.log2(math.e)
CHUNKS = 4
ROW_TILES = 24

f32 = jnp.float32
bf16 = jnp.bfloat16


def kernel(
    nb,
    q_hbm, kq_hbm, vq_hbm, k_hbm, v_hbm, len_hbm, off_hbm,
    out_ref,
    q_in, kq_in, vq_in, len_s, off_s, rows32, send_rows, got_q, got_kv, turn32,
    mine_q, all_q, keys, vals, parts, stats, own_o, own_l, got_o, got_l, row_o, last,
    mate_q, spare_q, first_q, first_o, first_l, pair_k, pair_v,
    loc, ex_send, ex_recv, s1_send, s1_recv, s2_send, s2_recv,
    r1_send, r1_recv, st_recv, r2_send, r2_recv,
    here, spare_recv, relay_recv, relay_send, first_send, first_recv, back_send, back_recv,
):
    rb = 2 * nb
    rows = rb * nb
    groups = max(rb // 8, 1)
    gs = rb // groups
    doc = k_hbm.shape[0]
    width = KVHALF * HD
    me = lax.axis_index("seq")
    c = lax.rem(me, 2)
    chip = me // 2
    x = lax.rem(chip, nb)
    y = chip // nb
    a = x * (1 - c) + y * c
    b = y * (1 - c) + x * c

    def dev(xx, yy, cc):
        return (yy * nb + xx) * 2 + cc

    def role_dev(aa, bb, cc):
        return dev(aa * (1 - c) + bb * c, bb * (1 - c) + aa * c, cc)

    def step(v, t):
        return lax.rem(v + t, nb)

    zero = me == 0
    rest = me > 0
    order = sorted(range(1, nb), key=lambda t: -min(t, nb - t))

    def send(src, dst, ssem, rsem, target):
        pltpu.make_async_remote_copy(
            src_ref=src, dst_ref=dst, send_sem=ssem, recv_sem=rsem,
            device_id={"seq": target}, device_id_type=pl.DeviceIdType.MESH,
        ).start()

    def await_bytes(ref, sem):
        pltpu.make_async_copy(ref, ref, sem).wait()

    mine = pl.ds(pl.multiple_of(c * width, 128), width)
    other = pl.ds(pl.multiple_of((1 - c) * width, 128), width)
    small = [
        pltpu.make_async_copy(q_hbm, q_in, loc.at[0]),
        pltpu.make_async_copy(kq_hbm, kq_in, loc.at[1]),
        pltpu.make_async_copy(vq_hbm, vq_in, loc.at[2]),
        pltpu.make_async_copy(len_hbm, len_s, loc.at[3]),
        pltpu.make_async_copy(off_hbm, off_s, loc.at[4]),
    ]
    large = [
        pltpu.make_async_copy(k_hbm.at[:, mine], keys.at[c], loc.at[5]),
        pltpu.make_async_copy(v_hbm.at[:, mine], vals.at[c], loc.at[6]),
    ]
    for copy in small:
        copy.start()
    mate = dev(x, y, 1 - c)

    def send_keys():
        send(k_hbm.at[:, other], keys.at[c], ex_send.at[0], ex_recv.at[0], mate)
        send(v_hbm.at[:, other], vals.at[c], ex_send.at[1], ex_recv.at[1], mate)

    barrier = pltpu.get_barrier_semaphore()

    def signal(sem, target):
        pl.semaphore_signal(
            sem, inc=1, device_id={"seq": target}, device_id_type=pl.DeviceIdType.MESH
        )

    @pl.when(rest)
    def _():
        for t in order:
            for cc in range(2):
                signal(barrier, dev(step(x, t), y, cc))
                signal(barrier, dev(x, step(y, t), cc))
        signal(barrier, dev(x, y, 1 - c))

    for copy in large:
        copy.start()
    for copy in small:
        copy.wait()
    for h in range(H):
        rows32[h : h + 1, :] = q_in[:, h * HD : (h + 1) * HD].astype(f32)
    for g in range(KVH):
        rows32[H + g : H + g + 1, :] = kq_in[:, g * HD : (g + 1) * HD].astype(f32)
        rows32[H + KVH + g : H + KVH + g + 1, :] = vq_in[:, g * HD : (g + 1) * HD].astype(f32)
    for r in range(2):
        send_rows[r, 0] = rows32[r * HALF : (r + 1) * HALF, :].astype(bf16)
        at = H + r * KVHALF
        send_rows[r, 1] = jnp.concatenate(
            [rows32[at : at + KVHALF, :], rows32[at + KVH : at + KVH + KVHALF, :]], axis=0
        ).astype(bf16)
    got_kv[a * 2 + c] = send_rows[c, 1]

    @pl.when(rest)
    def _():
        got_q[b * 2 + c] = send_rows[c, 0]

    @pl.when(a == 0)
    def _():
        got_q[0] = jnp.zeros((HALF, HD), bf16)

    @pl.when(me == 1)
    def _():
        mate_q[0] = jnp.zeros((HALF, HD), bf16)
        mate_q[1] = send_rows[0, 0]

    line = 4 * (nb - 1) + 1
    near = jnp.where((x == 0) | (y == 0), 1, 0)
    pl.semaphore_wait(barrier, jnp.where(zero, line, line - near))

    @pl.when(zero)
    def _():
        signal(here, 1)
        for t in order:
            for cc in range(2):
                signal(here, dev(t, 0, cc))
        send_keys()
        first_q[...] = send_rows[0, 0]
        for t in order:
            for cc in range(2):
                send(send_rows.at[cc, 0], first_q, first_send, first_recv, dev(t, 0, cc))
        send(send_rows.at[1, 0], first_q, first_send, first_recv, 1)
        for t in order:
            send(send_rows.at[0, 0], first_q, first_send, first_recv, dev(0, t, 0))

    line_peers = [(step(a, t), role_dev(step(a, t), b, c)) for t in order]
    my_block = pl.ds(pl.multiple_of(a * rb, rb), rb)
    per = HALF // CHUNKS

    def send_mate_row(k, slot):
        send(send_rows.at[1 - c, k], slot, s1_send.at[k], s1_recv.at[k], mate)

    @pl.when(rest)
    def _():
        for t in order:
            to_0 = dev(x, step(y, t), 0)

            @pl.when(to_0 > 0)
            def _(to_0=to_0):
                send(send_rows.at[0, 0], got_q.at[y * 2 + c], s1_send.at[0], s1_recv.at[0], to_0)

            @pl.when(to_0 == 0)
            def _():
                send(send_rows.at[0, 0], mate_q.at[y * 2 + c], s1_send.at[0], relay_recv, 1)

            send(
                send_rows.at[1, 0], got_q.at[x * 2 + c], s1_send.at[0], s1_recv.at[0],
                dev(step(x, t), y, 1),
            )

        @pl.when(me > 1)
        def _():
            send_mate_row(0, got_q.at[a * 2 + c])

    def send_row_0(target):
        send(send_rows.at[0, 1], got_kv.at[x * 2 + c], s1_send.at[1], s1_recv.at[1], target)

    for t in order:
        to_0 = dev(step(x, t), y, 0)

        @pl.when(to_0 > 0)
        def _(to_0=to_0):
            send_row_0(to_0)

        send(
            send_rows.at[1, 1], got_kv.at[y * 2 + c], s1_send.at[1], s1_recv.at[1],
            dev(x, step(y, t), 1),
        )

    @pl.when(me != 1)
    def _():
        send_mate_row(1, got_kv.at[b * 2 + c])

    @pl.when(me > 1)
    def _():
        send_keys()

    @pl.when(rest)
    def _():
        @pl.when(a == 0)
        def _():
            await_bytes(got_q.at[0 : rb - 2], s1_recv.at[0])

        @pl.when(a > 0)
        def _():
            await_bytes(got_q.at[0 : rb - 1], s1_recv.at[0])

        for i in range(rb):
            turn32[i * HALF : (i + 1) * HALF, :] = got_q[i].astype(f32)

    def turn(h):
        block = turn32[pl.ds(h, rb, stride=HALF), :].astype(bf16)
        mine_q[h] = block
        all_q[h, my_block, :] = block

    @pl.when((y > 0) | (me > 1) & (c == 1))
    def _():
        for j in range(CHUNKS):
            some = pl.ds(j * per, per)
            for h in range(j * per, (j + 1) * per):
                turn(h)
            for _, target in line_peers:
                send(mine_q.at[some], all_q.at[some, my_block, :], s2_send, s2_recv.at[j], target)

    @pl.when(me == 1)
    def _():
        for h in range(HALF):
            turn(h)
        await_bytes(mate_q.at[2:rb], relay_recv)
        for i in range(rb):
            turn32[i * HALF : (i + 1) * HALF, :] = mate_q[i].astype(f32)
        for h in range(HALF):
            spare_q[h, 0:rb, :] = turn32[pl.ds(h, rb, stride=HALF), :].astype(bf16)
        for j in range(CHUNKS):
            some = pl.ds(j * per, per)
            for t in order:
                send(
                    spare_q.at[some, 0:rb, :], all_q.at[some, 0:rb, :],
                    relay_send.at[0], s2_recv.at[j], dev(t, 0, 0),
                )
            for _, target in line_peers:
                send(mine_q.at[some], all_q.at[some, my_block, :], s2_send, s2_recv.at[j], target)

    @pl.when((y == 0) & (c == 0) & rest)
    def _():
        for h in range(HALF):
            turn(h)
        for j in range(CHUNKS):
            some = pl.ds(j * per, per)
            for _, target in line_peers:
                @pl.when(target > 0)
                def _(some=some, target=target, j=j):
                    send(
                        mine_q.at[some], all_q.at[some, my_block, :],
                        s2_send, s2_recv.at[j], target,
                    )

                @pl.when(target == 0)
                def _(some=some, j=j):
                    send(
                        mine_q.at[some], spare_q.at[some, my_block, :],
                        s2_send, spare_recv.at[j], 1,
                    )

    @pl.when((y == 0) & rest)
    def _():
        pl.semaphore_wait(here, 1)

        @pl.when(me == 1)
        def _():
            send_keys()
            send_mate_row(1, got_kv.at[b * 2 + c])

        @pl.when(me > 1)
        def _():
            send_row_0(0)

        await_bytes(first_q, first_recv)
        for t in order:
            send(first_q, first_q, first_send, first_recv, dev(x, t, c))

    lane = lax.broadcasted_iota(jnp.int32, (gs, 128), 1)
    for i in range(nb):
        stats[i] = jnp.full((gs, 128), NEG, f32)
    for copy in large:
        copy.wait()
    await_bytes(keys.at[1 - c], ex_recv.at[0])
    await_bytes(vals.at[1 - c], ex_recv.at[1])
    offset = off_s[0]
    places = lax.broadcasted_iota(jnp.int32, (1, doc), 1)
    seen = [places + (chip * 2 + blk) * doc < offset for blk in range(2)]
    ones = jnp.ones((doc, HD), bf16)

    def chunk(j, carry):
        first = j * per

        @pl.when(me == 1)
        def _():
            some = pl.ds(first, per)
            await_bytes(spare_q.at[some, rb:, :], spare_recv.at[j])
            send(spare_q.at[some], all_q.at[some], relay_send.at[1], s2_recv.at[j], 0)

        @pl.when(zero)
        def _():
            await_bytes(all_q.at[pl.ds(first, per)], s2_recv.at[j])

        @pl.when(rest)
        def _():
            await_bytes(all_q.at[pl.ds(first, per), 0 : (nb - 1) * rb, :], s2_recv.at[j])

        for u in range(per // GROUP):
            head = first + u * GROUP
            col = pl.ds(pl.multiple_of((head // GROUP) * HD, 128), HD)
            q = all_q[pl.ds(head, GROUP)].reshape(GROUP * rows, HD)
            tops, nums, dens = [], [], []
            for blk in range(2):
                s = lax.dot_general(
                    q, keys[blk, :, col], (((1,), (1,)), ((), ())), preferred_element_type=f32
                )
                s = jnp.where(seen[blk], s, NEG)
                top = jnp.max(s, axis=1, keepdims=True)
                p = jnp.exp2((s - top) * SCALE).astype(bf16)
                both = jnp.dot(
                    p, jnp.concatenate([vals[blk, :, col], ones], axis=1),
                    preferred_element_type=f32,
                )
                tops.append(top)
                nums.append(both[:, :HD])
                dens.append(both[:, HD:])
            top = jnp.maximum(tops[0], tops[1])
            w = [jnp.exp2((m - top) * SCALE) for m in tops]
            den = dens[0] * w[0] + dens[1] * w[1]
            inv = 1.0 / den
            o = nums[0] * (w[0] * inv) + nums[1] * (w[1] * inv)
            level = top * SCALE + jnp.log2(den)
            parts[pl.ds(head, GROUP)] = o.reshape(GROUP, rows, HD).astype(bf16)
            for i in range(nb):
                tile = stats[i]
                for z in range(GROUP):
                    for k in range(groups):
                        at = z * rows + i * rb + k * gs
                        tile = jnp.where(lane == k * HALF + head + z, level[at : at + gs], tile)
                stats[i] = tile
        for peer, target in line_peers:
            send(
                parts.at[pl.ds(first, per), pl.ds(pl.multiple_of(peer * rb, rb), rb), :],
                got_o.at[a, pl.ds(first, per)],
                r1_send.at[0], r1_recv.at[j], target,
            )

            @pl.when(j == CHUNKS - 1)
            def _(peer=peer, target=target):
                send(stats.at[peer], got_l.at[a], r1_send.at[1], st_recv, target)

        return carry

    lax.fori_loop(0, CHUNKS, chunk, 0)
    @pl.when(y > 0)
    def _():
        await_bytes(first_q, first_recv)

    head_of = lax.broadcasted_iota(jnp.int32, (HALF, HD), 0) // GROUP
    wide = jnp.concatenate(
        [jnp.where(head_of == g, first_q[...], jnp.zeros((), bf16)) for g in range(KVHALF)], axis=1
    )
    tops, nums, dens = [], [], []
    for blk in range(2):
        s = lax.dot_general(
            wide, keys[blk], (((1,), (1,)), ((), ())), preferred_element_type=f32
        )
        s = jnp.where(seen[blk], s, NEG)
        top = jnp.max(s, axis=1, keepdims=True)
        p = jnp.exp2((s - top) * SCALE).astype(bf16)
        dens.append(jnp.sum(p.astype(f32), axis=1, keepdims=True))
        num = jnp.dot(p, vals[blk], preferred_element_type=f32)
        pick = jnp.zeros((HALF, HD), f32)
        for g in range(KVHALF):
            pick = jnp.where(head_of == g, num[:, g * HD : (g + 1) * HD], pick)
        tops.append(top)
        nums.append(pick)
    top = jnp.maximum(tops[0], tops[1])
    w = [jnp.exp2((m - top) * SCALE) for m in tops]
    den = dens[0] * w[0] + dens[1] * w[1]
    level = top * SCALE + jnp.log2(den)
    half_lane = lax.broadcasted_iota(jnp.int32, (HALF // 2, 128), 1) < 64

    def paired(v):
        return jnp.where(half_lane, v[: HALF // 2], v[HALF // 2 :])

    first_o[a] = ((nums[0] * w[0] + nums[1] * w[1]) / den).astype(bf16)
    first_l[a] = paired(level)

    @pl.when(a > 0)
    def _():
        target = role_dev(0, b, c)
        send(first_o.at[a], first_o.at[a], back_send.at[0], back_recv.at[0], target)
        send(first_l.at[a], first_l.at[a], back_send.at[1], back_recv.at[1], target)

    await_bytes(got_kv.at[0 : rb - 1], s1_recv.at[1])
    for i in range(rb):
        turn32[i * HALF : (i + 1) * HALF, :] = got_kv[i].astype(f32)

    def row_of(aa, bb, cc):
        return dev(aa * (1 - c) + bb * c, bb * (1 - c) + aa * c, cc)

    spot = lax.rem(lax.broadcasted_iota(jnp.int32, (GROUP * rb, rb), 0), rb)
    key_spot = lax.broadcasted_iota(jnp.int32, (GROUP * rb, rb), 1)
    see = row_of(key_spot // 2, b, lax.rem(key_spot, 2)) <= row_of(a, spot // 2, lax.rem(spot, 2))
    own = jnp.full((gs, 128), NEG, f32)
    for g in range(KVHALF):
        key = turn32[pl.ds(g, rb, stride=HALF), :].astype(bf16)
        val = turn32[pl.ds(KVHALF + g, rb, stride=HALF), :].astype(bf16)
        q = all_q[g * GROUP : (g + 1) * GROUP, my_block, :].reshape(GROUP * rb, HD)
        s = lax.dot_general(q, key, (((1,), (1,)), ((), ())), preferred_element_type=f32)
        s = jnp.where(see, s, NEG)
        top = jnp.max(s, axis=1, keepdims=True)
        p = jnp.exp2((s - top) * SCALE).astype(bf16)
        den = jnp.sum(p.astype(f32), axis=1, keepdims=True)
        num = jnp.dot(p, val, preferred_element_type=f32)
        own_o[g * GROUP : (g + 1) * GROUP] = (num / den).reshape(GROUP, rb, HD)
        level = top * SCALE + jnp.log2(den)
        for i in range(GROUP):
            for k in range(groups):
                at = i * rb + k * gs
                own = jnp.where(lane == k * HALF + g * GROUP + i, level[at : at + gs], own)
    own_l[...] = own

    await_bytes(got_l.at[0 : nb - 1], st_recv)
    levels = [stats[a]] + [got_l[step(a, t)] for t in range(1, nb)] + [own_l[...]]
    top = functools.reduce(jnp.maximum, levels)
    weights = [jnp.exp2(v - top) for v in levels]
    total = functools.reduce(jnp.add, weights)
    inv = 1.0 / total
    weights = [w * inv for w in weights]
    level = top + jnp.log2(total)
    for j in range(CHUNKS):
        await_bytes(got_o.at[0 : nb - 1, pl.ds(j * per, per)], r1_recv.at[j])
        for h in range(j * per, (j + 1) * per):
            full = [parts[h, pl.ds(pl.multiple_of(a * rb, rb), rb), :].astype(f32)]
            full += [got_o[step(a, t), h].astype(f32) for t in range(1, nb)]
            full += [own_o[h]]
            for k in range(groups):
                at = k * HALF + h
                acc = weights[0][:, at : at + 1] * full[0][k * gs : (k + 1) * gs]
                for w, part in zip(weights[1:], full[1:]):
                    acc += w[:, at : at + 1] * part[k * gs : (k + 1) * gs]
                row_o[pl.ds(k * gs * ROW_TILES + h, gs, stride=ROW_TILES), :] = acc
    for h in range(HALF // 2):
        for k in range(groups):
            at = k * HALF + h
            pair = jnp.where(
                lane < 64, level[:, at : at + 1], level[:, at + HALF // 2 : at + HALF // 2 + 1]
            )
            row_o[pl.ds(k * gs * ROW_TILES + HALF + h, gs, stride=ROW_TILES), :] = pair

    def row_at(i):
        return pl.ds(pl.multiple_of(i * ROW_TILES, 8), ROW_TILES)

    def spread(w, k):
        return w[:, k * 64 : k * 64 + 1]

    def merged(levels, values):
        top = functools.reduce(jnp.maximum, levels)
        weights = [jnp.exp2(v - top) for v in levels]
        total = functools.reduce(jnp.add, weights)
        inv = 1.0 / total
        outs = []
        for k in range(2):
            terms = [
                spread(w * inv, k) * v[k * HALF // 2 : (k + 1) * HALF // 2]
                for w, v in zip(weights, values)
            ]
            outs.append(functools.reduce(jnp.add, terms))
        return jnp.concatenate(outs, axis=0), top + jnp.log2(total)

    mine_last = last.at[c * nb + b]
    for t in order:
        peer = step(b, t)
        for cc in range(2):
            target = role_dev(a, peer, cc)

            @pl.when(target > 0)
            def _(row=peer * 2 + cc, target=target):
                send(row_o.at[row_at(row)], mine_last, r2_send, r2_recv, target)

    @pl.when(me != 1)
    def _():
        send(row_o.at[row_at(b * 2 + 1 - c)], mine_last, r2_send, r2_recv, mate)

    mine_last[...] = row_o[row_at(b * 2 + c), :]

    @pl.when(a == 0)
    def _():
        await_bytes(first_o.at[0 : nb - 1], back_recv.at[0])
        await_bytes(first_l.at[0 : nb - 1], back_recv.at[1])
        pair = got_kv[0].astype(f32)
        for i in range(GROUP):
            pair_k[pl.ds(i, KVHALF, stride=GROUP), :] = pair[:KVHALF]
            pair_v[pl.ds(i, KVHALF, stride=GROUP), :] = pair[KVHALF:]
        score = jnp.sum(first_q[...].astype(f32) * pair_k[...], axis=1, keepdims=True) * SCALE
        score = jnp.where(jnp.full((HALF // 2, 128), b, jnp.int32) == 0, paired(score), NEG)
        values, level = merged(
            [first_l[i] for i in range(nb)] + [score],
            [first_o[i].astype(f32) for i in range(nb)] + [pair_v[...]],
        )
        row_o[0:HALF, :] = values
        row_o[HALF:ROW_TILES, :] = level

        @pl.when(zero)
        def _():
            mine_last[...] = row_o[0:ROW_TILES, :]

        @pl.when(rest)
        def _():
            send(row_o.at[0:ROW_TILES], mine_last, r2_send, r2_recv, 0)

    await_bytes(last.at[0 : 2 * nb - 1], r2_recv)

    live = jnp.full((HALF, 128), me, jnp.int32) < len_s[0]
    for r in range(2):
        got = [last[r * nb + i] for i in range(nb)]
        values, _ = merged([v[HALF:] for v in got], [v[:HALF] for v in got])
        out_ref[r * HALF : (r + 1) * HALF, :] = jnp.where(live, values, 0.0).astype(bf16)

    @pl.when(me == 1)
    def _():
        await_bytes(got_q.at[0 : rb - 2], s1_send.at[0])

    @pl.when(me > 1)
    def _():
        await_bytes(got_q.at[0 : rb - 1], s1_send.at[0])

    await_bytes(got_kv.at[0 : rb - 1], s1_send.at[1])
    for i, buf in enumerate((keys, vals)):
        await_bytes(buf.at[c], ex_send.at[i])
    await_bytes(got_o.at[0 : nb - 1], r1_send.at[0])
    await_bytes(got_l.at[0 : nb - 1], r1_send.at[1])

    @pl.when(rest)
    def _():
        await_bytes(all_q.at[:, 0 : (nb - 1) * rb, :], s2_send)

    @pl.when(a > 0)
    def _():
        await_bytes(first_o.at[a], back_send.at[0])
        await_bytes(first_l.at[a], back_send.at[1])

    @pl.when(me == 1)
    def _():
        await_bytes(all_q.at[:, rb:, :], relay_send.at[0])
        await_bytes(all_q, relay_send.at[1])

    await_bytes(last.at[0 : 2 * nb - 1], r2_send)

    @pl.when(zero)
    def _():
        await_bytes(got_q.at[0 : rb - 1], first_send)

    @pl.when(y == 0)
    def _():
        await_bytes(got_q.at[0 : nb - 1], first_send)


def local(nb, q, kq, vq, k, v, lengths, offsets):
    rb = 2 * nb
    rows = rb * nb
    doc = k.shape[0]
    gs = rb // max(rb // 8, 1)
    dma = pltpu.SemaphoreType.DMA
    out = pl.pallas_call(
        functools.partial(kernel, nb),
        out_shape=pltpu.VMEM((H, HD), bf16),
        in_specs=[pl.BlockSpec(memory_space=pltpu.HBM)] * 7,
        out_specs=pl.BlockSpec(memory_space=pltpu.VMEM),
        scratch_shapes=[
            pltpu.VMEM((1, H * HD), bf16),
            pltpu.VMEM((1, KVH * HD), bf16),
            pltpu.VMEM((1, KVH * HD), bf16),
            pltpu.SMEM((1,), jnp.int32),
            pltpu.SMEM((1,), jnp.int32),
            pltpu.VMEM((H + 2 * KVH, HD), f32),
            pltpu.VMEM((2, 2, HALF, HD), bf16),
            pltpu.VMEM((rb, HALF, HD), bf16),
            pltpu.VMEM((rb, HALF, HD), bf16),
            pltpu.VMEM((rb * HALF, HD), f32),
            pltpu.VMEM((HALF, rb, HD), bf16),
            pltpu.VMEM((HALF, rows, HD), bf16),
            pltpu.VMEM((2, doc, KVHALF * HD), bf16),
            pltpu.VMEM((2, doc, KVHALF * HD), bf16),
            pltpu.VMEM((HALF, rows, HD), bf16),
            pltpu.VMEM((nb, gs, 128), f32),
            pltpu.VMEM((HALF, rb, HD), f32),
            pltpu.VMEM((gs, 128), f32),
            pltpu.VMEM((nb, HALF, rb, HD), bf16),
            pltpu.VMEM((nb, gs, 128), f32),
            pltpu.VMEM((rb * ROW_TILES, HD), f32),
            pltpu.VMEM((2 * nb, ROW_TILES, HD), f32),
            pltpu.VMEM((rb, HALF, HD), bf16),
            pltpu.VMEM((HALF, rows, HD), bf16),
            pltpu.VMEM((HALF, HD), bf16),
            pltpu.VMEM((nb, HALF, HD), bf16),
            pltpu.VMEM((nb, HALF // 2, HD), f32),
            pltpu.VMEM((HALF, HD), f32),
            pltpu.VMEM((HALF, HD), f32),
            dma((7,)), dma((2,)), dma((2,)), dma((2,)), dma((2,)), dma, dma((CHUNKS,)),
            dma((2,)), dma((CHUNKS,)), dma, dma, dma,
            pltpu.SemaphoreType.REGULAR, dma((CHUNKS,)), dma, dma((2,)), dma, dma, dma((2,)), dma((2,)),
        ],
        compiler_params=pltpu.CompilerParams(
            collective_id=0, has_side_effects=True, vmem_limit_bytes=56 * 1024 * 1024
        ),
    )(q, kq, vq, k, v, lengths, offsets)
    return out.reshape(1, H * HD)


def solution(mesh):
    nb = math.isqrt(mesh.shape["seq"] // 2)
    rows = P(("grp", "seq"), None)
    return jax.shard_map(
        functools.partial(local, nb),
        mesh=mesh,
        in_specs=(rows, rows, rows, rows, rows, P("grp"), P("grp")),
        out_specs=rows,
        check_vma=False,
    )
```
